128 devices in a mesh: node: 4 (over y), torus: 32 (over z, x, core).
Axes of the slice: x: 4, y: 4, z: 4, core: 2. Of those that a mesh axis runs over, the one named last changes fastest.
Arguments:
- tokens: bfloat16 [16384, 7168], P(('node', 'torus')), may hold values from -6 to 6
- expert_ids: int32 [16384, 8], P(('node', 'torus')), may hold values from 0 to 383, as said below
- route_weight: bfloat16 [16384, 8], P(('node', 'torus')), may hold values from 0.19921875 to 2.5
- w_gate: bfloat16 [64, 7168, 1024], P('torus', None, 'node'), may hold values from -0.0625 to 0.0625
- w_up: bfloat16 [64, 7168, 1024], P('torus', None, 'node'), may hold values from -0.0625 to 0.0625
- w_down: bfloat16 [64, 1024, 7168], P('torus', 'node'), may hold values from -0.1875 to 0.1875
Outputs:
- moe_out: bfloat16 [16384, 7168], P(('node', 'torus'))
The draws below stay inside these ranges and needn't reach their ends.
Inputs may be any that keep to these rules, and one draw needn't show every extreme that they name: `expert_ids`: each row names 8 different experts. Counting an expert e below 64 as one of group e // 2, at most 4 of the 128 rows of one device (aligned blocks of rows, in order) name an expert of any one group, and in every draw some group is named by exactly 4 rows of every device.
All inputs are finite; a program needn't handle non-finite values.
Results may differ from the reference program's by a relative error of at most 0.0095.
Values may be sent and summed in bfloat16 or wider, within the bound.
A program may use at most 128 MiB of HBM per device.

```python
import math
import jax
import jax.numpy as jnp
from jax import lax

D = 7168
FF = 1024
EXPERTS = 384
TOPK = 8
EXP_DEV = 2
CAP = 4
QBLOCK = 128
TOK_DEV = 128
GROUPS = 32
SOURCES = 128
WIN_EXPERTS = 64
TOKENS = 16384
N_NODE = 4


def draw_expert_ids(key, part):
    keys = jax.random.split(jax.random.fold_in(key, 17), 8)
    group_ids = jnp.arange(GROUPS, dtype=jnp.int32)
    hot_group = jax.random.randint(keys[0], (), 0, GROUPS, dtype=jnp.int32)
    second_group = jax.random.randint(keys[1], (SOURCES,), 0, GROUPS, dtype=jnp.int32)
    second_used = jax.random.randint(keys[2], (SOURCES,), 0, 2, dtype=jnp.int32)
    counts = jax.random.randint(keys[3], (SOURCES, GROUPS), 1, 4, dtype=jnp.int32)
    counts = jnp.where(group_ids[None, :] == hot_group, CAP, counts)
    counts = jnp.where((group_ids[None, :] == second_group[:, None]) & (second_used[:, None] == 1), CAP, counts)
    ends = jnp.cumsum(counts, axis=1).astype(jnp.int32)
    laps = TOPK // EXP_DEV
    position = jnp.arange(laps * TOK_DEV, dtype=jnp.int32).reshape(laps, TOK_DEV)
    owner = jnp.sum((ends[:, None, None, :] <= position[None, :, :, None]).astype(jnp.int32), axis=-1)
    inside = position[None, :, :] < ends[:, -1][:, None, None]
    picked = jax.random.randint(keys[4], (SOURCES, laps, TOK_DEV), 0, 3, dtype=jnp.int32)
    first = EXP_DEV * owner + (picked == 1).astype(jnp.int32)
    second = EXP_DEV * owner + 1
    first = jnp.where(inside, first, -1)
    second = jnp.where(inside & (picked == 2), second, -1)
    paired = jnp.stack([first, second], axis=2)
    slots = paired.reshape(SOURCES, TOPK, TOK_DEV).transpose(0, 2, 1)
    shuffles = jax.vmap(lambda sub: jax.random.permutation(sub, TOK_DEV))(jax.random.split(keys[5], SOURCES))
    inverse = jnp.argsort(shuffles, axis=1).astype(jnp.int32)
    slots = jnp.take_along_axis(slots, inverse[:, :, None], axis=1)
    remain = EXPERTS - WIN_EXPERTS
    offset = jax.random.randint(keys[6], (SOURCES, TOK_DEV, 1), 0, remain, dtype=jnp.int32)
    filler = WIN_EXPERTS + (offset + jnp.arange(TOPK, dtype=jnp.int32)[None, None, :]) % remain
    chosen = jnp.where(slots >= 0, slots, filler)
    scores = jax.random.randint(keys[7], (SOURCES, TOK_DEV, TOPK), 0, 1 << 20, dtype=jnp.int32) * TOPK + jnp.arange(TOPK, dtype=jnp.int32)[None, None, :]
    order = jnp.argsort(scores, axis=-1, stable=True)
    chosen = jnp.take_along_axis(chosen, order, axis=-1)
    return chosen.reshape(TOKENS, TOPK).astype(jnp.int32)


def steps_of(stream_key, dims, cuts, least, high):
    gain, own = 1.0, jax.random.fold_in(stream_key, 6)
    for axis_at, shards_of in cuts:
        draws = jnp.exp(jax.random.uniform(jax.random.fold_in(own, axis_at), (shards_of,), jnp.float32, least / len(cuts), high / len(cuts)))
        gain = gain * jnp.repeat(draws, dims[axis_at] // shards_of).reshape([-1 if axis == axis_at else 1 for axis in range(len(dims))])
    return gain


def centred(stream_key, shape, width, bound, cuts=(), held_as=jnp.bfloat16):
    loudness = steps_of(stream_key, shape, cuts, -0.22, 0.18) if cuts else 1.0
    drawn = jax.random.normal(stream_key, shape, jnp.float32) * width * loudness
    return jnp.minimum(jnp.maximum(drawn, -bound), bound).astype(held_as)


def setup_inputs(seed: int = 0) -> dict:
    streams_of = jax.random.split(jax.random.key(seed), 7)
    tokens = centred(streams_of[0], (TOKENS, D), 1.0, 6.0, ((0, 128),))
    expert_ids = draw_expert_ids(jax.random.fold_in(streams_of[6], 71), 0)
    route_weight = jnp.clip(jnp.exp(math.log(2.5) - 2.5296425 * jax.random.uniform(streams_of[2], (TOKENS, TOPK), jnp.float32) ** steps_of(streams_of[2], (TOKENS, TOPK), ((0, 128),), -0.2, 0.2)), 0.19921875, 2.5).astype(jnp.bfloat16)
    w_gate = centred(streams_of[3], (WIN_EXPERTS, D, FF), D ** -0.5, 0.0625, ((0, 32), (2, 4)))
    w_up = centred(streams_of[4], (WIN_EXPERTS, D, FF), D ** -0.5, 0.0625, ((0, 32), (2, 4)))
    w_down = centred(streams_of[5], (WIN_EXPERTS, FF, D), FF ** -0.5, 0.1875, ((0, 32), (1, 4)))
    return {"tokens": tokens, "expert_ids": expert_ids, "route_weight": route_weight, "w_gate": w_gate, "w_up": w_up, "w_down": w_down}


block_rows = 64


def quantize(tokens):
    count = tokens.shape[0]
    blocks = tokens.astype(jnp.float32).reshape(count, -1, QBLOCK)
    largest = jnp.max(jnp.abs(blocks), axis=-1)
    scale = ((largest + 1e-6) * (1.0 / 448.0)).astype(jnp.bfloat16)
    scale = lax.optimization_barrier(scale)
    quantized = (blocks / scale.astype(jnp.float32)[:, :, None]).astype(jnp.bfloat16)
    quantized = lax.optimization_barrier(quantized)
    return quantized.reshape(count, -1), scale


def restore(quantized, scale):
    count = quantized.shape[0]
    blocks = quantized.astype(jnp.float32).reshape(count, -1, QBLOCK) * scale.astype(jnp.float32)[:, :, None]
    return blocks.astype(jnp.bfloat16).reshape(count, -1)


def reference(tokens, expert_ids, route_weight, w_gate, w_up, w_down):
    quantized, scale = quantize(tokens)
    restored = restore(quantized, scale)
    experts = jnp.arange(WIN_EXPERTS, dtype=jnp.int32)
    weight_float = route_weight.astype(jnp.float32)
    route_sel = jnp.zeros((TOKENS, WIN_EXPERTS), jnp.float32)
    named = jnp.zeros((TOKENS, WIN_EXPERTS), jnp.int32)
    for slot in range(TOPK):
        matched = expert_ids[:, slot:slot + 1] == experts[None, :]
        route_sel = route_sel + jnp.where(matched, weight_float[:, slot:slot + 1], jnp.float32(0.0))
        named = named + matched.astype(jnp.int32)
    member = named.reshape(TOKENS, GROUPS, EXP_DEV).sum(axis=-1)
    route_sel = route_sel.reshape(TOKENS, GROUPS, EXP_DEV)
    quarter = FF // N_NODE
    total = jnp.zeros((TOKENS, D), jnp.float32)
    offsets = jnp.arange(block_rows, dtype=jnp.int32)

    def group_step(group, total):
        inside = lax.dynamic_index_in_dim(member, group, 1, keepdims=False) > 0
        count = jnp.sum(inside.astype(jnp.int32)).astype(jnp.int32)
        order = jnp.argsort(jnp.where(inside, 0, 1).astype(jnp.int32), stable=True).astype(jnp.int32)
        order = jnp.concatenate([order, jnp.zeros((block_rows,), jnp.int32)])
        weights_group = lax.dynamic_index_in_dim(route_sel, group, 1, keepdims=False)
        gates = [lax.dynamic_index_in_dim(w_gate, EXP_DEV * group + expert, 0, keepdims=False) for expert in range(EXP_DEV)]
        ups = [lax.dynamic_index_in_dim(w_up, EXP_DEV * group + expert, 0, keepdims=False) for expert in range(EXP_DEV)]
        downs = [lax.dynamic_index_in_dim(w_down, EXP_DEV * group + expert, 0, keepdims=False) for expert in range(EXP_DEV)]

        def block_step(block, total):
            start = (block * block_rows).astype(jnp.int32)
            picked = lax.dynamic_slice_in_dim(order, start, block_rows)
            valid = (start + offsets) < count
            rows = restored[picked]
            weights = weights_group[picked]
            parts = [jnp.zeros((block_rows, D), jnp.float32) for piece in range(N_NODE)]
            for expert in range(EXP_DEV):
                gate = jnp.dot(rows, gates[expert], preferred_element_type=jnp.float32)
                upper = jnp.dot(rows, ups[expert], preferred_element_type=jnp.float32)
                hidden = (jax.nn.silu(gate) * upper).astype(jnp.bfloat16)
                for piece in range(N_NODE):
                    lower = piece * quarter
                    result = jnp.dot(hidden[:, lower:lower + quarter], downs[expert][lower:lower + quarter, :], preferred_element_type=jnp.float32)
                    parts[piece] = parts[piece] + weights[:, expert:expert + 1] * result
            combined = jnp.zeros((block_rows, D), jnp.float32)
            for piece in range(N_NODE):
                rounded = lax.optimization_barrier(parts[piece].astype(jnp.bfloat16))
                combined = combined + rounded.astype(jnp.float32)
            combined = lax.optimization_barrier(combined.astype(jnp.bfloat16))
            added = jnp.where(valid[:, None], combined.astype(jnp.float32), jnp.float32(0.0))
            return total.at[picked].add(added)

        blocks = (count + block_rows - 1) // block_rows
        return lax.fori_loop(0, blocks, block_step, total)

    total = lax.fori_loop(0, GROUPS, group_step, total)
    return total.astype(jnp.bfloat16)
```

```python
import functools

import jax
import jax.numpy as jnp
from jax import lax
from jax.experimental import pallas as pl
from jax.experimental.pallas import tpu as pltpu
from jax.sharding import PartitionSpec as P

EXP_DEV = 2
CAP = 4
QBLOCK = 128
LANES = 128
CHUNK = 1024
MESH = pl.DeviceIdType.MESH
F32 = jnp.float32
BF16 = jnp.bfloat16

TOK, PS, PR, YRS, YRR, YLS, YLR, XRS, XRR, XLS, XLR = range(11)
ORS, ORR, OLS, OLR, NRS, NRR, NLS, NLR, RS, RR, WT, OUT = range(11, 23)
N_SEMS = 23


def dot(a, b):
    return jnp.dot(a, b, preferred_element_type=F32)


def layer(
    nodes,
    groups,
    tok_hbm,
    ids_ref,
    rw_ref,
    wg_hbm,
    wu_hbm,
    wd_hbm,
    out_hbm,
    tok,
    wg,
    wu,
    wd,
    sbuf,
    rbuf,
    xbuf,
    wsb,
    wrb,
    wx,
    acc,
    hid,
    opr,
    opl,
    opr_in,
    opl_in,
    nbr,
    nbl,
    nbr_in,
    nbl_in,
    rsb,
    rrb,
    outv,
    place_ref,
    place_t_ref,
    sems,
):
    chunks, rows_tok, width = tok.shape
    slots = groups * CAP
    half = slots // 2
    ff = wg.shape[2]
    me_n = lax.axis_index("node")
    me_t = lax.axis_index("torus")
    right = (lax.rem(me_n + 1, nodes), me_t)
    left = (lax.rem(me_n + nodes - 1, nodes), me_t)

    def plane_peer(r):
        return (me_n, lax.rem(me_t + r, groups))

    def remote(src, dst, send, recv, device):
        return pltpu.make_async_remote_copy(
            src_ref=src,
            dst_ref=dst,
            send_sem=send,
            recv_sem=recv,
            device_id=device,
            device_id_type=MESH,
        )

    def spread(src, dst, send, recv):
        def one(r, carry):
            remote(src.at[r], dst.at[groups - r], send, recv, plane_peer(r)).start()
            return carry

        lax.fori_loop(1, groups, one, 0)

    def spread_desc(src, dst, send, recv):
        return remote(
            src.at[pl.ds(1, groups - 1)], dst.at[pl.ds(1, groups - 1)], send, recv, plane_peer(1)
        )

    barrier = pltpu.get_barrier_semaphore()

    def hello(r, carry):
        pl.semaphore_signal(barrier, inc=1, device_id=plane_peer(r), device_id_type=MESH)
        return carry

    lax.fori_loop(1, groups, hello, 0)
    pl.semaphore_signal(barrier, inc=1, device_id=right, device_id_type=MESH)
    pl.semaphore_signal(barrier, inc=1, device_id=left, device_id_type=MESH)

    def tok_copy(c):
        return pltpu.make_async_copy(
            tok_hbm.at[:, pl.ds(pl.multiple_of(c * width, width), width)],
            tok.at[c],
            sems.at[TOK, c],
        )

    def wd_copy(c):
        return pltpu.make_async_copy(
            wd_hbm.at[:, pl.ds(pl.multiple_of(c * width, width), width)],
            wd.at[c],
            sems.at[WT, c],
        )

    wg_copy = pltpu.make_async_copy(wg_hbm, wg, sems.at[TOK, chunks])
    wu_copy = pltpu.make_async_copy(wu_hbm, wu, sems.at[WT, chunks])
    for c in range(chunks):
        tok_copy(c).start()
    wg_copy.start()
    wu_copy.start()
    for c in range(chunks):
        wd_copy(c).start()

    slot = lax.broadcasted_iota(jnp.int32, (rows_tok, slots), 1)
    row = lax.broadcasted_iota(jnp.int32, (rows_tok, slots), 0)
    group = lax.rem(me_t + (slot >> 2), groups)
    ids = ids_ref[...]
    weights = rw_ref[...].astype(F32)
    member = jnp.zeros((rows_tok, slots), F32)
    weight_a = jnp.zeros((rows_tok, slots), F32)
    weight_b = jnp.zeros((rows_tok, slots), F32)
    for k in range(ids.shape[1]):
        one = jnp.broadcast_to(ids[:, k : k + 1], (rows_tok, slots))
        gain = jnp.broadcast_to(weights[:, k : k + 1], (rows_tok, slots))
        is_a = one == 2 * group
        is_b = one == 2 * group + 1
        weight_a = jnp.where(is_a, gain, weight_a)
        weight_b = jnp.where(is_b, gain, weight_b)
        member = jnp.where(is_a | is_b, jnp.float32(1.0), member)
    before = (
        lax.broadcasted_iota(jnp.int32, (rows_tok, rows_tok), 1)
        < lax.broadcasted_iota(jnp.int32, (rows_tok, rows_tok), 0)
    )
    before = jnp.where(before, jnp.float32(1.0), jnp.float32(0.0)).astype(BF16)
    index = dot(before, member.astype(BF16))
    here = index == (slot & (CAP - 1)).astype(F32)
    place_t = jnp.where(here, member, jnp.float32(0.0))
    place_t_ref[...] = place_t.astype(BF16)
    place_ref[...] = jnp.transpose(place_t).astype(BF16)
    lane = lax.broadcasted_iota(jnp.int32, (rows_tok, LANES), 1)
    low = jnp.where(lane < LANES // 2, jnp.float32(1.0), jnp.float32(0.0))
    spread_w = dot(jnp.transpose(place_t * weight_a).astype(BF16), low.astype(BF16)) + dot(
        jnp.transpose(place_t * weight_b).astype(BF16), (1.0 - low).astype(BF16)
    )
    wsb[...] = spread_w.reshape(groups, CAP, LANES).astype(BF16)

    def prepare(c):
        tok_copy(c).wait()
        parts = []
        for b in range(width // QBLOCK):
            x = tok[c, :, b * QBLOCK : (b + 1) * QBLOCK].astype(F32)
            top = jnp.max(jnp.abs(x), axis=1, keepdims=True)
            scale = ((top + 1e-06) * (1.0 / 448.0)).astype(BF16).astype(F32)
            scale = jnp.broadcast_to(scale, x.shape)
            quantized = (x / scale).astype(BF16)
            parts.append((quantized.astype(F32) * scale).astype(BF16))
        restored = jnp.concatenate(parts, axis=1)
        rows = dot(place_ref[...], restored)
        sbuf[c] = rows.reshape(groups, CAP, width).astype(BF16)

    def send_plane(c):
        spread(sbuf.at[c], rbuf.at[c], sems.at[PS, c], sems.at[PR, c])

    def y_send(block, c):
        return (
            remote(block.at[0], block.at[3], sems.at[YRS, c], sems.at[YRR, c], right),
            remote(block.at[0], block.at[1], sems.at[YLS, c], sems.at[YLR, c], left),
        )

    def y_relay(block, c):
        low_rows, high_rows = pl.ds(0, half), pl.ds(half, half)
        return (
            remote(
                block.at[3, low_rows], block.at[2, low_rows], sems.at[XRS, c], sems.at[XRR, c], right
            ),
            remote(
                block.at[1, high_rows], block.at[2, high_rows], sems.at[XLS, c], sems.at[XLR, c], left
            ),
        )

    def arrive(send, arrived, block, c):
        spread_desc(send, arrived, sems.at[PS, c], sems.at[PR, c]).wait_recv()
        arrived[0] = send[0]
        rows = arrived[...].astype(F32).reshape(slots, arrived.shape[2])
        block[0] = rows.astype(BF16)
        for copy in y_send(block, c):
            copy.start()

    def pass_on(block, c):
        for copy in y_send(block, c):
            copy.wait_recv()
        for copy in y_relay(block, c):
            copy.start()

    def multiply(c):
        for copy in y_relay(xbuf.at[c], c):
            copy.wait_recv()
        x = xbuf[c].reshape(nodes * slots, width)
        at = pl.ds(pl.multiple_of(c * width, width), width)
        for e in range(EXP_DEV):
            acc[2 * e] += dot(x, wg[e, at, :])
            acc[2 * e + 1] += dot(x, wu[e, at, :])

    acc[...] = jnp.zeros_like(acc)
    prepare(0)
    pl.semaphore_wait(barrier, groups + 1)
    send_plane(0)
    spread(wsb, wrb, sems.at[PS, chunks], sems.at[PR, chunks])

    def dispatch(s, carry):
        @pl.when((s >= 1) & (s < chunks))
        def _():
            prepare(s)
            send_plane(s)

        @pl.when((s >= 2) & (s < chunks + 2))
        def _():
            arrive(sbuf.at[s - 2], rbuf.at[s - 2], xbuf.at[s - 2], s - 2)

        @pl.when((s >= 4) & (s < chunks + 4))
        def _():
            pass_on(xbuf.at[s - 4], s - 4)

        @pl.when(s == 4)
        def _():
            wg_copy.wait()
            wu_copy.wait()
            arrive(wsb, wrb, wx, chunks)

        @pl.when(s == 6)
        def _():
            pass_on(wx, chunks)

        @pl.when(s >= 5)
        def _():
            multiply(s - 5)

        return carry

    lax.fori_loop(0, chunks + 5, dispatch, 0)
    for copy in y_relay(wx, chunks):
        copy.wait_recv()

    w_all = wx[...].reshape(nodes * slots, LANES).astype(F32)
    for e in range(EXP_DEV):
        gate = acc[2 * e]
        gain = jnp.broadcast_to(w_all[:, e * (LANES // 2) : e * (LANES // 2) + 1], gate.shape)
        value = gate / (1.0 + jnp.exp(-gate)) * acc[2 * e + 1] * gain
        hid[:, e * ff : (e + 1) * ff] = value.astype(BF16)

    def opposite(c):
        return (
            remote(opr.at[c], opr_in.at[c], sems.at[ORS, c], sems.at[ORR, c], right),
            remote(opl.at[c], opl_in.at[c], sems.at[OLS, c], sems.at[OLR, c], left),
        )

    def neighbour(c):
        return (
            remote(nbr.at[c], nbr_in.at[c], sems.at[NRS, c], sems.at[NRR, c], right),
            remote(nbl.at[c], nbl_in.at[c], sems.at[NLS, c], sems.at[NLR, c], left),
        )

    def start_opposite(c):
        wd_copy(c).wait()
        part = dot(hid[2 * slots : 3 * slots, :], wd[c])
        opr[c] = part[:half].astype(BF16)
        opl[c] = part[half:].astype(BF16)
        for copy in opposite(c):
            copy.start()

    def start_neighbour(c):
        for copy in opposite(c):
            copy.wait_recv()
        part = dot(hid[slots : 2 * slots, :], wd[c])
        nbr[c, :half] = (part[:half] + opr_in[c].astype(F32)).astype(BF16)
        nbr[c, half:] = part[half:].astype(BF16)
        part = dot(hid[3 * slots :, :], wd[c])
        nbl[c, :half] = part[:half].astype(BF16)
        nbl[c, half:] = (part[half:] + opl_in[c].astype(F32)).astype(BF16)
        for copy in neighbour(c):
            copy.start()

    def finish(c):
        for copy in neighbour(c):
            copy.wait_recv()
        part = dot(hid[:slots, :], wd[c])
        part = part + nbr_in[c].astype(F32) + nbl_in[c].astype(F32)
        rsb[c] = part.reshape(groups, CAP, width).astype(BF16)
        spread(rsb.at[c], rrb.at[c], sems.at[RS, c], sems.at[RR, c])

    def out_copy(c):
        return pltpu.make_async_copy(
            outv.at[c],
            out_hbm.at[:, pl.ds(pl.multiple_of(c * width, width), width)],
            sems.at[OUT, c],
        )

    def collect(c):
        spread_desc(rsb.at[c], rrb.at[c], sems.at[RS, c], sems.at[RR, c]).wait_recv()
        rrb[c, 0] = rsb[c, 0]
        back = rrb[c].astype(F32).reshape(slots, width).astype(BF16)
        outv[c] = dot(place_t_ref[...], back).astype(BF16)
        out_copy(c).start()

    def give_back(s, carry):
        @pl.when(s < chunks)
        def _():
            start_opposite(s)

        @pl.when((s >= 2) & (s < chunks + 2))
        def _():
            start_neighbour(s - 2)

        @pl.when((s >= 4) & (s < chunks + 4))
        def _():
            finish(s - 4)

        @pl.when(s >= 6)
        def _():
            collect(s - 6)

        return carry

    lax.fori_loop(0, chunks + 6, give_back, 0)

    def drain(c, carry):
        spread_desc(sbuf.at[c], rbuf.at[c], sems.at[PS, c], sems.at[PR, c]).wait_send()
        spread_desc(rsb.at[c], rrb.at[c], sems.at[RS, c], sems.at[RR, c]).wait_send()
        for copy in y_send(xbuf.at[c], c) + y_relay(xbuf.at[c], c) + opposite(c) + neighbour(c):
            copy.wait_send()
        out_copy(c).wait()
        return carry

    lax.fori_loop(0, chunks, drain, 0)
    spread_desc(wsb, wrb, sems.at[PS, chunks], sems.at[PR, chunks]).wait_send()
    for copy in y_send(wx, chunks) + y_relay(wx, chunks):
        copy.wait_send()


def solution(mesh):
    nodes, groups = mesh.shape["node"], mesh.shape["torus"]

    def shards(tokens, expert_ids, route_weight, w_gate, w_up, w_down):
        rows_tok, depth = tokens.shape
        ff = w_gate.shape[2]
        width = min(CHUNK, depth)
        chunks = depth // width
        slots = groups * CAP
        half = slots // 2
        anywhere = pl.BlockSpec(memory_space=pl.ANY)
        inside = pl.BlockSpec(memory_space=pltpu.VMEM)
        block = pltpu.VMEM((chunks, groups, CAP, width), BF16)
        halves = pltpu.VMEM((chunks, half, width), BF16)
        whole = pltpu.VMEM((chunks, slots, width), BF16)
        return pl.pallas_call(
            functools.partial(layer, nodes, groups),
            out_shape=jax.ShapeDtypeStruct((rows_tok, depth), BF16),
            in_specs=[anywhere, inside, inside, anywhere, anywhere, anywhere],
            out_specs=anywhere,
            scratch_shapes=[
                pltpu.VMEM((chunks, rows_tok, width), BF16),
                pltpu.VMEM(w_gate.shape, BF16),
                pltpu.VMEM(w_up.shape, BF16),
                pltpu.VMEM((chunks, EXP_DEV * ff, width), BF16),
                block,
                block,
                pltpu.VMEM((chunks, nodes, slots, width), BF16),
                pltpu.VMEM((groups, CAP, LANES), BF16),
                pltpu.VMEM((groups, CAP, LANES), BF16),
                pltpu.VMEM((nodes, slots, LANES), BF16),
                pltpu.VMEM((2 * EXP_DEV, nodes * slots, ff), F32),
                pltpu.VMEM((nodes * slots, EXP_DEV * ff), BF16),
                halves,
                halves,
                halves,
                halves,
                whole,
                whole,
                whole,
                whole,
                block,
                block,
                pltpu.VMEM((chunks, rows_tok, width), BF16),
                pltpu.VMEM((slots, rows_tok), BF16),
                pltpu.VMEM((rows_tok, slots), BF16),
                pltpu.SemaphoreType.DMA((N_SEMS, chunks + 1)),
            ],
            compiler_params=pltpu.CompilerParams(
                collective_id=0, has_side_effects=True, vmem_limit_bytes=67043328
            ),
        )(
            tokens,
            expert_ids,
            route_weight,
            w_gate,
            w_up,
            w_down.reshape(EXP_DEV * ff, depth),
        )

    placed = (
        P(("node", "torus"), None),
        P(("node", "torus"), None),
        P(("node", "torus"), None),
        P("torus", None, "node"),
        P("torus", None, "node"),
        P("torus", "node", None),
    )
    return jax.shard_map(
        shards, mesh=mesh, in_specs=placed, out_specs=P(("node", "torus"), None), check_vma=False
    )
```

```python
import functools

import jax
import jax.numpy as jnp
from jax import lax
from jax.experimental import pallas as pl
from jax.experimental.pallas import tpu as pltpu
from jax.sharding import PartitionSpec as P

EXP_DEV = 2
CAP = 4
QBLOCK = 128
LANES = 128
CHUNK = 1024
BATCHES = 2
MESH = pl.DeviceIdType.MESH
F32 = jnp.float32
BF16 = jnp.bfloat16

TOK, PS, PR, YRS, YRR, YLS, YLR, XRS, XRR, XLS, XLR = range(11)
ORS, ORR, OLS, OLR, NRS, NRR, NLS, NLR, RS, RR, WT, OUT = range(11, 23)
N_SEMS = 23


def dot(a, b):
    return jnp.dot(a, b, preferred_element_type=F32)


def layer(
    nodes,
    groups,
    tok_hbm,
    ids_ref,
    rw_ref,
    wg_hbm,
    wu_hbm,
    wd_hbm,
    out_hbm,
    tok,
    wg,
    wu,
    wd,
    sbuf,
    rbuf,
    xbuf,
    wsb,
    wrb,
    wx,
    acc,
    hid,
    opr,
    opl,
    opr_in,
    opl_in,
    nbr,
    nbl,
    nbr_in,
    nbl_in,
    rsb,
    rrb,
    outv,
    place_ref,
    place_t_ref,
    sems,
):
    chunks, rows_tok, width = tok.shape
    steps = BATCHES * chunks
    some = groups // BATCHES
    slots = groups * CAP
    rows = some * CAP
    half = rows // 2
    ff = wg.shape[2]
    me_n = lax.axis_index("node")
    me_t = lax.axis_index("torus")
    right = (lax.rem(me_n + 1, nodes), me_t)
    left = (lax.rem(me_n + nodes - 1, nodes), me_t)
    OWN, RIGHT, LEFT, FAR = range(4)

    def plane_peer(r):
        return (me_n, lax.rem(me_t + r, groups))

    def remote(src, dst, send, recv, device):
        return pltpu.make_async_remote_copy(
            src_ref=src,
            dst_ref=dst,
            send_sem=send,
            recv_sem=recv,
            device_id=device,
            device_id_type=MESH,
        )

    def spread(src, dst, send, recv, batch):
        def one(j, carry):
            peer = plane_peer(BATCHES * j + batch)
            remote(src.at[j], dst.at[some - batch - j], send, recv, peer).start()
            return carry

        lax.fori_loop(1 - batch, some, one, 0)

    def spread_desc(src, dst, send, recv, low, high):
        at = pl.ds(low, high - low)
        return remote(src.at[at], dst.at[at], send, recv, plane_peer(1))

    def spread_wait(src, dst, send, recv, batch, received):
        for b in range(BATCHES):

            @pl.when(batch == b)
            def _(b=b):
                copy = spread_desc(src, dst, send, recv, 1 - b, some)
                if received:
                    copy.wait_recv()
                else:
                    copy.wait_send()

    barrier = pltpu.get_barrier_semaphore()

    def hello(r, carry):
        pl.semaphore_signal(barrier, inc=1, device_id=plane_peer(r), device_id_type=MESH)
        return carry

    lax.fori_loop(1, groups, hello, 0)
    pl.semaphore_signal(barrier, inc=1, device_id=right, device_id_type=MESH)
    pl.semaphore_signal(barrier, inc=1, device_id=left, device_id_type=MESH)

    def tok_copy(c):
        return pltpu.make_async_copy(
            tok_hbm.at[:, pl.ds(pl.multiple_of(c * width, width), width)],
            tok.at[c],
            sems.at[TOK, c],
        )

    def wd_copy(c):
        return pltpu.make_async_copy(
            wd_hbm.at[:, pl.ds(pl.multiple_of(c * width, width), width)],
            wd.at[c],
            sems.at[WT, c],
        )

    wg_copy = pltpu.make_async_copy(wg_hbm, wg, sems.at[TOK, chunks])
    wu_copy = pltpu.make_async_copy(wu_hbm, wu, sems.at[WT, chunks])
    for c in range(chunks):
        tok_copy(c).start()
    wg_copy.start()
    wu_copy.start()
    for c in range(chunks):
        wd_copy(c).start()

    slot = lax.broadcasted_iota(jnp.int32, (slots, rows_tok), 0)
    spot = slot // CAP
    offset = BATCHES * lax.rem(spot, some) + spot // some
    group = lax.rem(me_t + offset, groups)
    ids = ids_ref[...]
    weights = rw_ref[...].astype(F32)
    member = jnp.zeros((slots, rows_tok), F32)
    weight_a = jnp.zeros((slots, rows_tok), F32)
    weight_b = jnp.zeros((slots, rows_tok), F32)
    for k in range(ids.shape[0]):
        one = jnp.broadcast_to(ids[k : k + 1, :], (slots, rows_tok))
        gain = jnp.broadcast_to(weights[k : k + 1, :], (slots, rows_tok))
        is_a = one == 2 * group
        is_b = one == 2 * group + 1
        weight_a = jnp.where(is_a, gain, weight_a)
        weight_b = jnp.where(is_b, gain, weight_b)
        member = jnp.where(is_a | is_b, jnp.float32(1.0), member)
    before = (
        lax.broadcasted_iota(jnp.int32, (rows_tok, rows_tok), 0)
        < lax.broadcasted_iota(jnp.int32, (rows_tok, rows_tok), 1)
    )
    before = jnp.where(before, jnp.float32(1.0), jnp.float32(0.0)).astype(BF16)
    index = dot(member.astype(BF16), before)
    here = index == lax.rem(slot, CAP).astype(F32)
    place = jnp.where(here, member, jnp.float32(0.0))
    place_ref[...] = place.astype(BF16)
    place_t_ref[...] = jnp.transpose(place).astype(BF16)
    lane = lax.broadcasted_iota(jnp.int32, (rows_tok, LANES), 1)
    low = jnp.where(lane < LANES // 2, jnp.float32(1.0), jnp.float32(0.0))
    spread_w = dot((place * weight_a).astype(BF16), low.astype(BF16)) + dot(
        (place * weight_b).astype(BF16), (1.0 - low).astype(BF16)
    )
    wsb[...] = spread_w.reshape(groups, CAP, LANES).astype(BF16)

    def prepare(c):
        tok_copy(c).wait()
        parts = []
        for b in range(width // QBLOCK):
            x = tok[c, :, b * QBLOCK : (b + 1) * QBLOCK].astype(F32)
            top = jnp.max(jnp.abs(x), axis=1, keepdims=True)
            scale = ((top + 1e-06) * (1.0 / 448.0)).astype(BF16).astype(F32)
            scale = jnp.broadcast_to(scale, x.shape)
            quantized = (x / scale).astype(BF16)
            parts.append((quantized.astype(F32) * scale).astype(BF16))
        restored = jnp.concatenate(parts, axis=1)
        picked = dot(place_ref[...], restored).reshape(groups, CAP, width).astype(BF16)
        for b in range(BATCHES):
            sbuf[b * chunks + c] = picked[b * some : (b + 1) * some]

    def send_plane(u):
        spread(sbuf.at[u], rbuf.at[u], sems.at[PS, u], sems.at[PR, u], u // chunks)

    def y_send(block, u):
        return (
            remote(block.at[OWN], block.at[LEFT], sems.at[YRS, u], sems.at[YRR, u], right),
            remote(block.at[OWN], block.at[RIGHT], sems.at[YLS, u], sems.at[YLR, u], left),
        )

    def y_relay(block, u):
        middle = block.shape[1] // 2
        low, high = pl.ds(0, middle), pl.ds(middle, middle)
        return (
            remote(block.at[LEFT, low], block.at[FAR, low], sems.at[XRS, u], sems.at[XRR, u], right),
            remote(block.at[RIGHT, high], block.at[FAR, high], sems.at[XLS, u], sems.at[XLR, u], left),
        )

    def flat(ref_value):
        count, cap, lanes = ref_value.shape
        return ref_value.astype(F32).reshape(count * cap, lanes).astype(BF16)

    def arrive(u):
        batch = u // chunks
        spread_wait(sbuf.at[u], rbuf.at[u], sems.at[PS, u], sems.at[PR, u], batch, True)

        @pl.when(batch == 0)
        def _():
            rbuf[u, 0] = sbuf[u, 0]

        xbuf[u, OWN] = flat(rbuf[u])
        for copy in y_send(xbuf.at[u], u):
            copy.start()

    def pass_on(block, u):
        for copy in y_send(block, u):
            copy.wait_recv()
        for copy in y_relay(block, u):
            copy.start()

    def multiply(u):
        for copy in y_relay(xbuf.at[u], u):
            copy.wait_recv()
        batch = u // chunks
        x = xbuf[u].reshape(nodes * rows, width)
        at = pl.ds(pl.multiple_of((u - batch * chunks) * width, width), width)
        for e in range(EXP_DEV):
            acc[batch, 2 * e] += dot(x, wg[e, at, :])
            acc[batch, 2 * e + 1] += dot(x, wu[e, at, :])

    def activate(batch):
        w_all = wx[:, pl.ds(pl.multiple_of(batch * rows, rows), rows), :]
        w_all = w_all.astype(F32).reshape(nodes * rows, LANES)
        for e in range(EXP_DEV):
            gate = acc[batch, 2 * e]
            gain = jnp.broadcast_to(w_all[:, e * (LANES // 2) : e * (LANES // 2) + 1], gate.shape)
            value = gate / (1.0 + jnp.exp(-gate)) * acc[batch, 2 * e + 1] * gain
            hid[batch, :, e * ff : (e + 1) * ff] = value.astype(BF16)

    def opposite(u):
        return (
            remote(opr.at[u], opr_in.at[u], sems.at[ORS, u], sems.at[ORR, u], right),
            remote(opl.at[u], opl_in.at[u], sems.at[OLS, u], sems.at[OLR, u], left),
        )

    def neighbour(u):
        return (
            remote(nbr.at[u], nbr_in.at[u], sems.at[NRS, u], sems.at[NRR, u], right),
            remote(nbl.at[u], nbl_in.at[u], sems.at[NLS, u], sems.at[NLR, u], left),
        )

    def project(u, first, count):
        batch = u // chunks
        return dot(hid[batch, first * rows : (first + count) * rows, :], wd[u - batch * chunks])

    def start_opposite(u):
        @pl.when(u < chunks)
        def _():
            wd_copy(u).wait()

        part = project(u, FAR, 1)
        opr[u] = part[:half].astype(BF16)
        opl[u] = part[half:].astype(BF16)
        for copy in opposite(u):
            copy.start()

    def start_neighbour(u):
        part = project(u, RIGHT, 2)
        for copy in opposite(u):
            copy.wait_recv()
        nbr[u, :half] = (part[:half] + opr_in[u].astype(F32)).astype(BF16)
        nbr[u, half:] = part[half:rows].astype(BF16)
        nbl[u, :half] = part[rows : rows + half].astype(BF16)
        nbl[u, half:] = (part[rows + half :] + opl_in[u].astype(F32)).astype(BF16)
        for copy in neighbour(u):
            copy.start()

    def finish(u):
        part = project(u, OWN, 1)
        for copy in neighbour(u):
            copy.wait_recv()
        part = part + nbr_in[u].astype(F32) + nbl_in[u].astype(F32)
        rsb[u] = part.reshape(some, CAP, width).astype(BF16)
        spread(rsb.at[u], rrb.at[u], sems.at[RS, u], sems.at[RR, u], u // chunks)

    def out_copy(c):
        return pltpu.make_async_copy(
            outv.at[c],
            out_hbm.at[:, pl.ds(pl.multiple_of(c * width, width), width)],
            sems.at[OUT, c],
        )

    def collect(c):
        total = jnp.zeros((rows_tok, width), F32)
        for b in range(BATCHES):
            u = b * chunks + c
            spread_desc(
                rsb.at[u], rrb.at[u], sems.at[RS, u], sems.at[RR, u], 1 - b, some
            ).wait_recv()
            if b == 0:
                rrb[u, 0] = rsb[u, 0]
            total += dot(place_t_ref[:, b * rows : (b + 1) * rows], flat(rrb[u]))
        outv[c] = total.astype(BF16)
        out_copy(c).start()

    acc[...] = jnp.zeros_like(acc)
    prepare(0)
    pl.semaphore_wait(barrier, groups + 1)
    send_plane(0)
    for b in range(BATCHES):
        at = pl.ds(b * some, some)
        spread(wsb.at[at], wrb.at[at], sems.at[PS, steps], sems.at[PR, steps], b)

    lag_y, lag_x, lag_m = 2, 4, 5
    lag_o = steps + 1
    lag_n, lag_f, lag_c = lag_o + 2, lag_o + 4, lag_o + 6

    def stage(s, lag, first, last, work):
        @pl.when((s >= lag + first) & (s < lag + last))
        def _():
            work(s - lag)

    def whole(s, carry):
        stage(s, 0, 1, chunks, prepare)
        stage(s, 0, 1, steps, send_plane)
        stage(s, lag_y, 0, steps, arrive)

        @pl.when(s == 3)
        def _():
            spread_desc(wsb, wrb, sems.at[PS, steps], sems.at[PR, steps], 1, groups).wait_recv()
            wrb[0] = wsb[0]
            wx[OWN] = flat(wrb[...])
            for copy in y_send(wx, steps):
                copy.start()
            wg_copy.wait()
            wu_copy.wait()

        stage(s, lag_x, 0, steps, lambda u: pass_on(xbuf.at[u], u))

        @pl.when(s == 5)
        def _():
            pass_on(wx, steps)

        stage(s, lag_m, 0, steps, multiply)

        @pl.when(s == 7)
        def _():
            for copy in y_relay(wx, steps):
                copy.wait_recv()

        @pl.when((s == lag_m + chunks - 1) | (s == lag_m + steps - 1))
        def _():
            activate((s - lag_m) // chunks)

        stage(s, lag_o, 0, steps, start_opposite)
        stage(s, lag_n, 0, steps, start_neighbour)
        stage(s, lag_f, 0, steps, finish)
        stage(s, lag_c + steps - chunks, 0, chunks, collect)
        return carry

    lax.fori_loop(0, lag_c + steps, whole, 0)

    def drain(u, carry):
        spread_wait(sbuf.at[u], rbuf.at[u], sems.at[PS, u], sems.at[PR, u], u // chunks, False)
        spread_wait(rsb.at[u], rrb.at[u], sems.at[RS, u], sems.at[RR, u], u // chunks, False)
        for copy in y_send(xbuf.at[u], u) + y_relay(xbuf.at[u], u) + opposite(u) + neighbour(u):
            copy.wait_send()

        @pl.when(u < chunks)
        def _():
            out_copy(u).wait()

        return carry

    lax.fori_loop(0, steps, drain, 0)
    spread_desc(wsb, wrb, sems.at[PS, steps], sems.at[PR, steps], 1, groups).wait_send()
    for copy in y_send(wx, steps) + y_relay(wx, steps):
        copy.wait_send()


def solution(mesh):
    nodes, groups = mesh.shape["node"], mesh.shape["torus"]

    def shards(tokens, expert_ids, route_weight, w_gate, w_up, w_down):
        rows_tok, depth = tokens.shape
        ff = w_gate.shape[2]
        width = min(CHUNK, depth)
        chunks = depth // width
        slots = groups * CAP
        steps = BATCHES * chunks
        some = groups // BATCHES
        rows = some * CAP
        anywhere = pl.BlockSpec(memory_space=pl.ANY)
        inside = pl.BlockSpec(memory_space=pltpu.VMEM)
        block = pltpu.VMEM((steps, some, CAP, width), BF16)
        halves = pltpu.VMEM((steps, rows // 2, width), BF16)
        whole = pltpu.VMEM((steps, rows, width), BF16)
        return pl.pallas_call(
            functools.partial(layer, nodes, groups),
            out_shape=jax.ShapeDtypeStruct((rows_tok, depth), BF16),
            in_specs=[anywhere, inside, inside, anywhere, anywhere, anywhere],
            out_specs=anywhere,
            scratch_shapes=[
                pltpu.VMEM((chunks, rows_tok, width), BF16),
                pltpu.VMEM(w_gate.shape, BF16),
                pltpu.VMEM(w_up.shape, BF16),
                pltpu.VMEM((chunks, EXP_DEV * ff, width), BF16),
                block,
                block,
                pltpu.VMEM((steps, nodes, rows, width), BF16),
                pltpu.VMEM((groups, CAP, LANES), BF16),
                pltpu.VMEM((groups, CAP, LANES), BF16),
                pltpu.VMEM((nodes, slots, LANES), BF16),
                pltpu.VMEM((BATCHES, 2 * EXP_DEV, nodes * rows, ff), F32),
                pltpu.VMEM((BATCHES, nodes * rows, EXP_DEV * ff), BF16),
                halves,
                halves,
                halves,
                halves,
                whole,
                whole,
                whole,
                whole,
                block,
                block,
                pltpu.VMEM((chunks, rows_tok, width), BF16),
                pltpu.VMEM((slots, rows_tok), BF16),
                pltpu.VMEM((rows_tok, slots), BF16),
                pltpu.SemaphoreType.DMA((N_SEMS, steps + 1)),
            ],
            compiler_params=pltpu.CompilerParams(
                collective_id=0, has_side_effects=True, vmem_limit_bytes=67043328
            ),
        )(
            tokens,
            expert_ids.T,
            route_weight.T,
            w_gate,
            w_up,
            w_down.reshape(EXP_DEV * ff, depth),
        )

    placed = (
        P(("node", "torus"), None),
        P(("node", "torus"), None),
        P(("node", "torus"), None),
        P("torus", None, "node"),
        P("torus", None, "node"),
        P("torus", "node", None),
    )
    return jax.shard_map(
        shards, mesh=mesh, in_specs=placed, out_specs=P(("node", "torus"), None), check_vma=False
    )
```

```python
import functools

import jax
import jax.numpy as jnp
from jax import lax
from jax.experimental import pallas as pl
from jax.experimental.pallas import tpu as pltpu
from jax.sharding import PartitionSpec as P

EXP_DEV = 2
CAP = 4
QBLOCK = 128
LANES = 128
CHUNK = 1024
BATCHES = 2
MESH = pl.DeviceIdType.MESH
F32 = jnp.float32
BF16 = jnp.bfloat16

TOK, PS, PR, YRS, YRR, YLS, YLR, XRS, XRR, XLS, XLR = range(11)
ORS, ORR, OLS, OLR, NRS, NRR, NLS, NLR, RS, RR, WT, OUT = range(11, 23)
N_SEMS = 23


def dot(a, b):
    return jnp.dot(a, b, preferred_element_type=F32)


def layer(
    nodes,
    groups,
    tok_hbm,
    ids_ref,
    rw_ref,
    wg_hbm,
    wu_hbm,
    wd_hbm,
    out_hbm,
    tok,
    wg,
    wu,
    wd,
    sbuf,
    rbuf,
    xbuf,
    wsb,
    wrb,
    wx,
    acc,
    hid,
    opr,
    opl,
    opr_in,
    opl_in,
    nbr,
    nbl,
    nbr_in,
    nbl_in,
    rsb,
    rrb,
    zbuf,
    zin,
    wbuf,
    win,
    far_r,
    far_l,
    wnr,
    wnl,
    wnr_in,
    wnl_in,
    outv,
    place_ref,
    place_t_ref,
    sems,
    round_sems,
):
    chunks, rows_tok, width = tok.shape
    plain = chunks - 1
    steps = BATCHES * plain
    some = groups // BATCHES
    slots = groups * CAP
    rows = some * CAP
    half = rows // 2
    ff = wg.shape[2]
    me_n = lax.axis_index("node")
    me_t = lax.axis_index("torus")
    right = (lax.rem(me_n + 1, nodes), me_t)
    left = (lax.rem(me_n + nodes - 1, nodes), me_t)
    OWN, RIGHT, LEFT, FAR = range(4)

    def plane_peer(r):
        return (me_n, lax.rem(me_t + r, groups))

    def remote(src, dst, send, recv, device):
        return pltpu.make_async_remote_copy(
            src_ref=src,
            dst_ref=dst,
            send_sem=send,
            recv_sem=recv,
            device_id=device,
            device_id_type=MESH,
        )

    def spread(src, dst, send, recv, batch):
        def one(j, carry):
            peer = plane_peer(BATCHES * j + batch)
            remote(src.at[j], dst.at[some - batch - j], send, recv, peer).start()
            return carry

        lax.fori_loop(1 - batch, some, one, 0)

    def spread_desc(src, dst, send, recv, low, high):
        at = pl.ds(low, high - low)
        return remote(src.at[at], dst.at[at], send, recv, plane_peer(1))

    def spread_wait(src, dst, send, recv, batch, received):
        for b in range(BATCHES):

            @pl.when(batch == b)
            def _(b=b):
                copy = spread_desc(src, dst, send, recv, 1 - b, some)
                if received:
                    copy.wait_recv()
                else:
                    copy.wait_send()

    across = min(4, groups // 2)
    deep = groups // (2 * across)
    me_core, me_x, me_z = lax.rem(me_t, 2), lax.rem(me_t // 2, across), me_t // (2 * across)

    def torus_peer(dz, dx, dc):
        z, x, core = lax.rem(me_z + dz, deep), lax.rem(me_x + dx, across), lax.rem(me_core + dc, 2)
        return (me_n, (z * across + x) * 2 + core)

    partner = [torus_peer(0, 0, 1)]
    along_x = [torus_peer(0, 1, 0), torus_peer(0, across - 1, 0)]
    along_z = [torus_peer(1, 0, 0), torus_peer(deep - 1, 0, 0)] if deep > 1 else []
    barrier = pltpu.get_barrier_semaphore()
    greeted = [right, left] + partner + along_x + along_z
    for device in greeted:
        pl.semaphore_signal(barrier, inc=1, device_id=device, device_id_type=MESH)
    rounds = [along_x] + [along_z] * (2 if deep > 1 else 0) + [partner]

    def tell(k):
        for device in rounds[k]:
            pl.semaphore_signal(round_sems.at[k], inc=1, device_id=device, device_id_type=MESH)

    def told(k):
        pl.semaphore_wait(round_sems.at[k], len(rounds[k]))

    def tok_copy(c):
        return pltpu.make_async_copy(
            tok_hbm.at[:, pl.ds(pl.multiple_of(c * width, width), width)],
            tok.at[c],
            sems.at[TOK, c],
        )

    def wd_copy(c):
        return pltpu.make_async_copy(
            wd_hbm.at[:, pl.ds(pl.multiple_of(c * width, width), width)],
            wd.at[c],
            sems.at[WT, c],
        )

    wg_copy = pltpu.make_async_copy(wg_hbm, wg, sems.at[TOK, chunks])
    wu_copy = pltpu.make_async_copy(wu_hbm, wu, sems.at[WT, chunks])
    for c in range(chunks):
        tok_copy(c).start()
    wg_copy.start()
    wu_copy.start()
    for c in range(chunks):
        wd_copy(c).start()

    slot = lax.broadcasted_iota(jnp.int32, (slots, rows_tok), 0)
    spot = slot // CAP
    offset = BATCHES * lax.rem(spot, some) + spot // some
    group = lax.rem(me_t + offset, groups)
    ids = ids_ref[...]
    weights = rw_ref[...].astype(F32)
    member = jnp.zeros((slots, rows_tok), F32)
    weight_a = jnp.zeros((slots, rows_tok), F32)
    weight_b = jnp.zeros((slots, rows_tok), F32)
    for k in range(ids.shape[0]):
        one = jnp.broadcast_to(ids[k : k + 1, :], (slots, rows_tok))
        gain = jnp.broadcast_to(weights[k : k + 1, :], (slots, rows_tok))
        is_a = one == 2 * group
        is_b = one == 2 * group + 1
        weight_a = jnp.where(is_a, gain, weight_a)
        weight_b = jnp.where(is_b, gain, weight_b)
        member = jnp.where(is_a | is_b, jnp.float32(1.0), member)
    before = (
        lax.broadcasted_iota(jnp.int32, (rows_tok, rows_tok), 0)
        < lax.broadcasted_iota(jnp.int32, (rows_tok, rows_tok), 1)
    )
    before = jnp.where(before, jnp.float32(1.0), jnp.float32(0.0)).astype(BF16)
    index = dot(member.astype(BF16), before)
    here = index == lax.rem(slot, CAP).astype(F32)
    place = jnp.where(here, member, jnp.float32(0.0))
    place_ref[...] = place.astype(BF16)
    place_t_ref[...] = jnp.transpose(place).astype(BF16)
    lane = lax.broadcasted_iota(jnp.int32, (rows_tok, LANES), 1)
    low = jnp.where(lane < LANES // 2, jnp.float32(1.0), jnp.float32(0.0))
    spread_w = dot((place * weight_a).astype(BF16), low.astype(BF16)) + dot(
        (place * weight_b).astype(BF16), (1.0 - low).astype(BF16)
    )
    wsb[...] = spread_w.reshape(groups, CAP, LANES).astype(BF16)

    def prepare(c):
        tok_copy(c).wait()
        parts = []
        for b in range(width // QBLOCK):
            x = tok[c, :, b * QBLOCK : (b + 1) * QBLOCK].astype(F32)
            top = jnp.max(jnp.abs(x), axis=1, keepdims=True)
            scale = ((top + 1e-06) * (1.0 / 448.0)).astype(BF16).astype(F32)
            scale = jnp.broadcast_to(scale, x.shape)
            quantized = (x / scale).astype(BF16)
            parts.append((quantized.astype(F32) * scale).astype(BF16))
        restored = jnp.concatenate(parts, axis=1)
        picked = dot(place_ref[...], restored).reshape(groups, CAP, width).astype(BF16)
        if c == 0:
            zbuf[OWN] = picked
        else:
            for b in range(BATCHES):
                sbuf[b * plain + c - 1] = picked[b * some : (b + 1) * some]

    def send_plane(u):
        spread(sbuf.at[u], rbuf.at[u], sems.at[PS, u], sems.at[PR, u], u // plain)

    def y_send(block, u):
        return (
            remote(block.at[OWN], block.at[LEFT], sems.at[YRS, u], sems.at[YRR, u], right),
            remote(block.at[OWN], block.at[RIGHT], sems.at[YLS, u], sems.at[YLR, u], left),
        )

    def y_relay(block, u):
        middle = block.shape[1] // 2
        low, high = pl.ds(0, middle), pl.ds(middle, middle)
        return (
            remote(block.at[LEFT, low], block.at[FAR, low], sems.at[XRS, u], sems.at[XRR, u], right),
            remote(block.at[RIGHT, high], block.at[FAR, high], sems.at[XLS, u], sems.at[XLR, u], left),
        )

    def flat(ref_value):
        count, cap, lanes = ref_value.shape
        return ref_value.astype(F32).reshape(count * cap, lanes).astype(BF16)

    def arrive(u):
        batch = u // plain
        spread_wait(sbuf.at[u], rbuf.at[u], sems.at[PS, u], sems.at[PR, u], batch, True)

        @pl.when(batch == 0)
        def _():
            rbuf[u, 0] = sbuf[u, 0]

        xbuf[u, OWN] = flat(rbuf[u])
        for copy in y_send(xbuf.at[u], u):
            copy.start()

    def pass_on(block, u):
        for copy in y_send(block, u):
            copy.wait_recv()
        for copy in y_relay(block, u):
            copy.start()

    def multiply(u):
        for copy in y_relay(xbuf.at[u], u):
            copy.wait_recv()
        batch = u // plain
        add_chunk(xbuf[u].reshape(nodes * rows, width), batch, u - batch * plain + 1)

    def add_chunk(x, batch, c):
        at = pl.ds(pl.multiple_of(c * width, width), width)
        for e in range(EXP_DEV):
            acc[batch, 2 * e] += dot(x, wg[e, at, :])
            acc[batch, 2 * e + 1] += dot(x, wu[e, at, :])

    def z_piece(batch):
        return zbuf.at[:, pl.ds(batch * some, some)], steps + 1 + batch

    def spread_planes(src, dst, send, recv, batch):
        def one(j, carry):
            peer = plane_peer(BATCHES * j + batch)
            here, there = batch * some + j, batch * some + some - batch - j
            remote(src.at[:, here], dst.at[:, there], send, recv, peer).start()
            return carry

        lax.fori_loop(1 - batch, some, one, 0)

    def planes_desc(src, dst, send, recv, batch):
        at = pl.ds(batch * some + 1 - batch, some - 1 + batch)
        return remote(src.at[:, at], dst.at[:, at], send, recv, plane_peer(1))

    def z_plane(batch):
        u = steps + 1 + batch
        return zbuf, zin, sems.at[PS, u], sems.at[PR, u], batch

    def w_plane(batch):
        u = steps + 1 + batch
        return wbuf, win, sems.at[RS, u], sems.at[RR, u], batch

    def z_out(batch):
        for copy in y_relay(*z_piece(batch)):
            copy.wait_recv()
        spread_planes(*z_plane(batch))

    def z_multiply(batch):
        planes_desc(*z_plane(batch)).wait_recv()
        if batch == 0:
            zin[:, 0] = zbuf[:, 0]
        x = zin[:, batch * some : (batch + 1) * some].astype(F32)
        add_chunk(x.reshape(nodes * rows, width).astype(BF16), batch, 0)

    def w_project(batch):
        if batch == 0:
            wd_copy(plain).wait()
        part = dot(hid[batch], wd[plain])
        wbuf[:, batch * some : (batch + 1) * some] = part.reshape(nodes, some, CAP, width).astype(BF16)
        spread_planes(*w_plane(batch))

    def w_far(batch):
        u, mid = steps + 1 + batch, some // 2
        first, second = pl.ds(batch * some, mid), pl.ds(batch * some + mid, mid)
        return (
            remote(win.at[FAR, first], far_r.at[batch], sems.at[ORS, u], sems.at[ORR, u], right),
            remote(win.at[FAR, second], far_l.at[batch], sems.at[OLS, u], sems.at[OLR, u], left),
        )

    def w_near(batch):
        u = steps + 1 + batch
        return (
            remote(wnr.at[batch], wnr_in.at[batch], sems.at[NRS, u], sems.at[NRR, u], right),
            remote(wnl.at[batch], wnl_in.at[batch], sems.at[NLS, u], sems.at[NLR, u], left),
        )

    def w_opposite(batch):
        planes_desc(*w_plane(batch)).wait_recv()
        if batch == 0:
            win[:, 0] = wbuf[:, 0]
        for copy in w_far(batch):
            copy.start()

    def w_neighbour(batch):
        low, mid, high = batch * some, batch * some + some // 2, (batch + 1) * some
        for copy in w_far(batch):
            copy.wait_recv()
        wnr[batch, : some // 2] = (
            win[RIGHT, low:mid].astype(F32) + far_r[batch].astype(F32)
        ).astype(BF16)
        wnr[batch, some // 2 :] = win[RIGHT, mid:high]
        wnl[batch, : some // 2] = win[LEFT, low:mid]
        wnl[batch, some // 2 :] = (
            win[LEFT, mid:high].astype(F32) + far_l[batch].astype(F32)
        ).astype(BF16)
        for copy in w_near(batch):
            copy.start()

    def w_finish(batch):
        for copy in w_near(batch):
            copy.wait_recv()
        part = win[OWN, batch * some : (batch + 1) * some].astype(F32)
        part = part + wnr_in[batch].astype(F32) + wnl_in[batch].astype(F32)
        return dot(
            place_t_ref[:, batch * rows : (batch + 1) * rows], part.reshape(rows, width).astype(BF16)
        )

    def activate(batch):
        w_all = wx[:, pl.ds(pl.multiple_of(batch * rows, rows), rows), :]
        w_all = w_all.astype(F32).reshape(nodes * rows, LANES)
        for e in range(EXP_DEV):
            gate = acc[batch, 2 * e]
            gain = jnp.broadcast_to(w_all[:, e * (LANES // 2) : e * (LANES // 2) + 1], gate.shape)
            value = gate / (1.0 + jnp.exp(-gate)) * acc[batch, 2 * e + 1] * gain
            hid[batch, :, e * ff : (e + 1) * ff] = value.astype(BF16)

    def opposite(u):
        return (
            remote(opr.at[u], opr_in.at[u], sems.at[ORS, u], sems.at[ORR, u], right),
            remote(opl.at[u], opl_in.at[u], sems.at[OLS, u], sems.at[OLR, u], left),
        )

    def neighbour(u):
        return (
            remote(nbr.at[u], nbr_in.at[u], sems.at[NRS, u], sems.at[NRR, u], right),
            remote(nbl.at[u], nbl_in.at[u], sems.at[NLS, u], sems.at[NLR, u], left),
        )

    def project(u, first, count):
        batch = u // plain
        return dot(hid[batch, first * rows : (first + count) * rows, :], wd[u - batch * plain])

    def start_opposite(u):
        @pl.when(u < plain)
        def _():
            wd_copy(u).wait()

        part = project(u, FAR, 1)
        opr[u] = part[:half].astype(BF16)
        opl[u] = part[half:].astype(BF16)
        for copy in opposite(u):
            copy.start()

    def start_neighbour(u):
        part = project(u, RIGHT, 2)
        for copy in opposite(u):
            copy.wait_recv()
        nbr[u, :half] = (part[:half] + opr_in[u].astype(F32)).astype(BF16)
        nbr[u, half:] = part[half:rows].astype(BF16)
        nbl[u, :half] = part[rows : rows + half].astype(BF16)
        nbl[u, half:] = (part[rows + half :] + opl_in[u].astype(F32)).astype(BF16)
        for copy in neighbour(u):
            copy.start()

    def finish(u):
        part = project(u, OWN, 1)
        for copy in neighbour(u):
            copy.wait_recv()
        part = part + nbr_in[u].astype(F32) + nbl_in[u].astype(F32)
        rsb[u] = part.reshape(some, CAP, width).astype(BF16)
        spread(rsb.at[u], rrb.at[u], sems.at[RS, u], sems.at[RR, u], u // plain)

    def out_copy(c):
        return pltpu.make_async_copy(
            outv.at[c],
            out_hbm.at[:, pl.ds(pl.multiple_of(c * width, width), width)],
            sems.at[OUT, c],
        )

    def collect(c):
        total = jnp.zeros((rows_tok, width), F32)
        for b in range(BATCHES):
            u = b * plain + c
            spread_desc(
                rsb.at[u], rrb.at[u], sems.at[RS, u], sems.at[RR, u], 1 - b, some
            ).wait_recv()
            if b == 0:
                rrb[u, 0] = rsb[u, 0]
            total += dot(place_t_ref[:, b * rows : (b + 1) * rows], flat(rrb[u]))
        outv[c] = total.astype(BF16)
        out_copy(c).start()

    prepare(0)
    pl.semaphore_wait(barrier, len(greeted))
    for b in range(BATCHES):
        for copy in y_send(*z_piece(b)):
            copy.start()
    acc[...] = jnp.zeros_like(acc)
    for c in range(1, chunks):
        if c <= len(rounds):
            tell(c - 1)
        prepare(c)
        if c <= len(rounds):
            told(c - 1)
    for u in range(4):
        send_plane(u)
    for b in range(BATCHES):
        at = pl.ds(b * some, some)
        spread(wsb.at[at], wrb.at[at], sems.at[PS, steps], sems.at[PR, steps], b)
    for b in range(BATCHES):
        pass_on(*z_piece(b))

    lag_y, lag_x, lag_m = 0, 2, 4
    lag_o = steps + 1
    lag_n, lag_f, lag_c = lag_o + 2, lag_o + 4, lag_o + 6

    def stage(s, lag, first, last, work):
        @pl.when((s >= lag + first) & (s < lag + last))
        def _():
            work(s - lag)

    def at_step(s, step, work, *args):
        @pl.when(s == step)
        def _():
            work(*args)

    def share_weights():
        spread_desc(wsb, wrb, sems.at[PS, steps], sems.at[PR, steps], 1, groups).wait_recv()
        wrb[0] = wsb[0]
        wx[OWN] = flat(wrb[...])
        for copy in y_send(wx, steps):
            copy.start()

    def have_gate_up():
        wg_copy.wait()
        wu_copy.wait()

    def have_weights():
        for copy in y_relay(wx, steps):
            copy.wait_recv()

    def turn(batch):
        z_multiply(batch)
        activate(batch)
        w_project(batch)

    def w_last():
        total = w_finish(0) + w_finish(1)
        outv[plain] = total.astype(BF16)
        out_copy(plain).start()

    def send_two(k):
        send_plane(4 + 2 * k)
        send_plane(5 + 2 * k)

    def whole(s, carry):
        stage(s, 0, 0, (steps - 4) // 2, send_two)
        stage(s, lag_y, 0, steps, arrive)
        at_step(s, 1, share_weights)
        at_step(s, 3, have_gate_up)
        stage(s, lag_x, 0, steps, lambda u: pass_on(xbuf.at[u], u))
        at_step(s, 3, pass_on, wx, steps)
        at_step(s, 4, z_out, 0)
        at_step(s, 5, z_out, 1)
        stage(s, lag_m, 0, steps, multiply)
        at_step(s, 6, have_weights)
        at_step(s, steps, turn, 0)
        at_step(s, lag_m + steps - 1, turn, 1)
        stage(s, lag_o, 0, steps, start_opposite)
        at_step(s, lag_o + steps, w_opposite, 0)
        at_step(s, lag_o + steps + 1, w_opposite, 1)
        stage(s, lag_n, 0, steps, start_neighbour)
        at_step(s, lag_n + steps, w_neighbour, 0)
        at_step(s, lag_n + steps + 1, w_neighbour, 1)
        stage(s, lag_f, 0, steps, finish)
        stage(s, lag_c + steps - plain, 0, plain, collect)
        at_step(s, lag_f + steps + 1, w_last)
        return carry

    lax.fori_loop(0, lag_f + steps + 2, whole, 0)

    def drain(u, carry):
        spread_wait(sbuf.at[u], rbuf.at[u], sems.at[PS, u], sems.at[PR, u], u // plain, False)
        spread_wait(rsb.at[u], rrb.at[u], sems.at[RS, u], sems.at[RR, u], u // plain, False)
        for copy in y_send(xbuf.at[u], u) + y_relay(xbuf.at[u], u) + opposite(u) + neighbour(u):
            copy.wait_send()

        @pl.when(u < chunks)
        def _():
            out_copy(u).wait()

        return carry

    lax.fori_loop(0, steps, drain, 0)
    spread_desc(wsb, wrb, sems.at[PS, steps], sems.at[PR, steps], 1, groups).wait_send()
    for copy in y_send(wx, steps) + y_relay(wx, steps):
        copy.wait_send()
    for b in range(BATCHES):
        planes_desc(*z_plane(b)).wait_send()
        planes_desc(*w_plane(b)).wait_send()
        for copy in y_send(*z_piece(b)) + y_relay(*z_piece(b)) + w_far(b) + w_near(b):
            copy.wait_send()


def solution(mesh):
    nodes, groups = mesh.shape["node"], mesh.shape["torus"]

    def shards(tokens, expert_ids, route_weight, w_gate, w_up, w_down):
        rows_tok, depth = tokens.shape
        ff = w_gate.shape[2]
        width = min(CHUNK, depth)
        chunks = depth // width
        slots = groups * CAP
        steps = BATCHES * (chunks - 1)
        some = groups // BATCHES
        rows = some * CAP
        anywhere = pl.BlockSpec(memory_space=pl.ANY)
        inside = pl.BlockSpec(memory_space=pltpu.VMEM)
        block = pltpu.VMEM((steps, some, CAP, width), BF16)
        planes = pltpu.VMEM((nodes, groups, CAP, width), BF16)
        piece = pltpu.VMEM((BATCHES, some, CAP, width), BF16)
        halves = pltpu.VMEM((steps, rows // 2, width), BF16)
        whole = pltpu.VMEM((steps, rows, width), BF16)
        return pl.pallas_call(
            functools.partial(layer, nodes, groups),
            out_shape=jax.ShapeDtypeStruct((rows_tok, depth), BF16),
            in_specs=[anywhere, inside, inside, anywhere, anywhere, anywhere],
            out_specs=anywhere,
            scratch_shapes=[
                pltpu.VMEM((chunks, rows_tok, width), BF16),
                pltpu.VMEM(w_gate.shape, BF16),
                pltpu.VMEM(w_up.shape, BF16),
                pltpu.VMEM((chunks, EXP_DEV * ff, width), BF16),
                block,
                block,
                pltpu.VMEM((steps, nodes, rows, width), BF16),
                pltpu.VMEM((groups, CAP, LANES), BF16),
                pltpu.VMEM((groups, CAP, LANES), BF16),
                pltpu.VMEM((nodes, slots, LANES), BF16),
                pltpu.VMEM((BATCHES, 2 * EXP_DEV, nodes * rows, ff), F32),
                pltpu.VMEM((BATCHES, nodes * rows, EXP_DEV * ff), BF16),
                halves,
                halves,
                halves,
                halves,
                whole,
                whole,
                whole,
                whole,
                block,
                block,
                planes,
                planes,
                planes,
                planes,
                pltpu.VMEM((BATCHES, some // 2, CAP, width), BF16),
                pltpu.VMEM((BATCHES, some // 2, CAP, width), BF16),
                piece,
                piece,
                piece,
                piece,
                pltpu.VMEM((chunks, rows_tok, width), BF16),
                pltpu.VMEM((slots, rows_tok), BF16),
                pltpu.VMEM((rows_tok, slots), BF16),
                pltpu.SemaphoreType.DMA((N_SEMS, steps + 1 + BATCHES)),
                pltpu.SemaphoreType.REGULAR((4,)),
            ],
            compiler_params=pltpu.CompilerParams(
                collective_id=0, has_side_effects=True, vmem_limit_bytes=67043328
            ),
        )(
            tokens,
            expert_ids.T,
            route_weight.T,
            w_gate,
            w_up,
            w_down.reshape(EXP_DEV * ff, depth),
        )

    placed = (
        P(("node", "torus"), None),
        P(("node", "torus"), None),
        P(("node", "torus"), None),
        P("torus", None, "node"),
        P("torus", None, "node"),
        P("torus", "node", None),
    )
    return jax.shard_map(
        shards, mesh=mesh, in_specs=placed, out_specs=P(("node", "torus"), None), check_vma=False
    )
```

```python
import functools

import jax
import jax.numpy as jnp
from jax import lax
from jax.experimental import pallas as pl
from jax.experimental.pallas import tpu as pltpu
from jax.sharding import PartitionSpec as P

EXP_DEV = 2
CAP = 4
QBLOCK = 128
LANES = 128
CHUNK = 1024
BATCHES = 2
EARLY = 4
MESH = pl.DeviceIdType.MESH
F32 = jnp.float32
BF16 = jnp.bfloat16

TOK, PS, PR, YRS, YRR, YLS, YLR, XRS, XRR, XLS, XLR = range(11)
ORS, ORR, OLS, OLR, NRS, NRR, NLS, NLR, RS, RR, WT, OUT = range(11, 23)
N_SEMS = 23


def dot(a, b):
    return jnp.dot(a, b, preferred_element_type=F32)


def layer(
    nodes,
    groups,
    tok_hbm,
    ids_ref,
    rw_ref,
    wg_hbm,
    wu_hbm,
    wd_hbm,
    out_ref,
    tok,
    wg,
    wu,
    wd,
    sbuf,
    rbuf,
    xbuf,
    wsb,
    wrb,
    wx,
    acc,
    hid,
    opr,
    opl,
    opr_in,
    opl_in,
    nbr,
    nbl,
    nbr_in,
    nbl_in,
    rsb,
    rrb,
    zbuf,
    zin,
    wbuf,
    win,
    far_r,
    far_l,
    wnr,
    wnl,
    wnr_in,
    wnl_in,
    place_ref,
    place_t_ref,
    sems,
    round_sem,
):
    chunks, rows_tok, width = tok.shape
    plain = chunks - 1
    steps = BATCHES * plain
    some = groups // BATCHES
    slots = groups * CAP
    rows = some * CAP
    half = rows // 2
    ff = wg.shape[2]
    me_n = lax.axis_index("node")
    me_t = lax.axis_index("torus")
    right = (lax.rem(me_n + 1, nodes), me_t)
    left = (lax.rem(me_n + nodes - 1, nodes), me_t)
    OWN, RIGHT, LEFT, FAR = range(4)

    def plane_peer(r):
        return (me_n, lax.rem(me_t + r, groups))

    def remote(src, dst, send, recv, device):
        return pltpu.make_async_remote_copy(
            src_ref=src,
            dst_ref=dst,
            send_sem=send,
            recv_sem=recv,
            device_id=device,
            device_id_type=MESH,
        )

    def spread(src, dst, send, recv, batch):
        def one(j, carry):
            peer = plane_peer(BATCHES * j + batch)
            remote(src.at[j], dst.at[some - batch - j], send, recv, peer).start()
            return carry

        lax.fori_loop(1 - batch, some, one, 0)

    def spread_desc(src, dst, send, recv, low, high):
        at = pl.ds(low, high - low)
        return remote(src.at[at], dst.at[at], send, recv, plane_peer(1))

    def spread_wait(src, dst, send, recv, batch, received):
        for b in range(BATCHES):

            @pl.when(batch == b)
            def _(b=b):
                copy = spread_desc(src, dst, send, recv, 1 - b, some)
                if received:
                    copy.wait_recv()
                else:
                    copy.wait_send()

    across = min(4, groups // 2)
    deep = groups // (2 * across)
    me_core, me_x, me_z = lax.rem(me_t, 2), lax.rem(me_t // 2, across), me_t // (2 * across)

    def torus_peer(dz, dx, dc):
        z, x, core = lax.rem(me_z + dz, deep), lax.rem(me_x + dx, across), lax.rem(me_core + dc, 2)
        return (me_n, (z * across + x) * 2 + core)

    beside = [torus_peer(0, dx, 0) for dx in range(1, across)]
    greeted = [right, left, torus_peer(0, 0, 1)] + beside
    greeted += [torus_peer(0, dx, 1) for dx in range(1, across)]
    greeted += [torus_peer(dz, 0, dc) for dz in range(1, deep) for dc in range(2)]
    barrier = pltpu.get_barrier_semaphore()
    for device in greeted:
        pl.semaphore_signal(barrier, inc=1, device_id=device, device_id_type=MESH)

    def tok_copy(c):
        return pltpu.make_async_copy(
            tok_hbm.at[:, pl.ds(pl.multiple_of(c * width, width), width)],
            tok.at[c],
            sems.at[TOK, c],
        )

    def wd_copy(c):
        return pltpu.make_async_copy(
            wd_hbm.at[:, pl.ds(pl.multiple_of(c * width, width), width)],
            wd.at[c],
            sems.at[WT, c],
        )

    wg_copy = pltpu.make_async_copy(wg_hbm, wg, sems.at[TOK, chunks])
    wu_copy = pltpu.make_async_copy(wu_hbm, wu, sems.at[WT, chunks])
    for c in range(chunks):
        tok_copy(c).start()
    wg_copy.start()
    wu_copy.start()
    for c in range(chunks):
        wd_copy(c).start()

    slot = lax.broadcasted_iota(jnp.int32, (slots, rows_tok), 0)
    spot = slot // CAP
    offset = BATCHES * lax.rem(spot, some) + spot // some
    group = lax.rem(me_t + offset, groups)
    ids = ids_ref[...]
    weights = rw_ref[...].astype(F32)
    member = jnp.zeros((slots, rows_tok), F32)
    weight_a = jnp.zeros((slots, rows_tok), F32)
    weight_b = jnp.zeros((slots, rows_tok), F32)
    for k in range(ids.shape[0]):
        one = jnp.broadcast_to(ids[k : k + 1, :], (slots, rows_tok))
        gain = jnp.broadcast_to(weights[k : k + 1, :], (slots, rows_tok))
        is_a = one == 2 * group
        is_b = one == 2 * group + 1
        weight_a = jnp.where(is_a, gain, weight_a)
        weight_b = jnp.where(is_b, gain, weight_b)
        member = jnp.where(is_a | is_b, jnp.float32(1.0), member)
    before = (
        lax.broadcasted_iota(jnp.int32, (rows_tok, rows_tok), 0)
        < lax.broadcasted_iota(jnp.int32, (rows_tok, rows_tok), 1)
    )
    before = jnp.where(before, jnp.float32(1.0), jnp.float32(0.0)).astype(BF16)
    index = dot(member.astype(BF16), before)
    here = index == lax.rem(slot, CAP).astype(F32)
    place = jnp.where(here, member, jnp.float32(0.0))
    place_ref[...] = place.astype(BF16)
    place_t_ref[...] = jnp.transpose(place).astype(BF16)
    lane = lax.broadcasted_iota(jnp.int32, (rows_tok, LANES), 1)
    low = jnp.where(lane < LANES // 2, jnp.float32(1.0), jnp.float32(0.0))
    spread_w = dot((place * weight_a).astype(BF16), low.astype(BF16)) + dot(
        (place * weight_b).astype(BF16), (1.0 - low).astype(BF16)
    )
    wsb[...] = spread_w.reshape(groups, CAP, LANES).astype(BF16)

    def prepare(c):
        tok_copy(c).wait()
        parts = []
        for b in range(width // QBLOCK):
            x = tok[c, :, b * QBLOCK : (b + 1) * QBLOCK].astype(F32)
            top = jnp.max(jnp.abs(x), axis=1, keepdims=True)
            scale = ((top + 1e-06) * (1.0 / 448.0)).astype(BF16).astype(F32)
            scale = jnp.broadcast_to(scale, x.shape)
            quantized = (x / scale).astype(BF16)
            parts.append((quantized.astype(F32) * scale).astype(BF16))
        restored = jnp.concatenate(parts, axis=1)
        picked = dot(place_ref[...], restored).reshape(groups, CAP, width).astype(BF16)
        if c == 0:
            zbuf[OWN] = picked
        else:
            for b in range(BATCHES):
                sbuf[b * plain + c - 1] = picked[b * some : (b + 1) * some]

    def send_plane(u):
        spread(sbuf.at[u], rbuf.at[u], sems.at[PS, u], sems.at[PR, u], u // plain)

    def y_send(block, u):
        return (
            remote(block.at[OWN], block.at[LEFT], sems.at[YRS, u], sems.at[YRR, u], right),
            remote(block.at[OWN], block.at[RIGHT], sems.at[YLS, u], sems.at[YLR, u], left),
        )

    def y_relay(block, u):
        middle = block.shape[1] // 2
        low, high = pl.ds(0, middle), pl.ds(middle, middle)
        return (
            remote(block.at[LEFT, low], block.at[FAR, low], sems.at[XRS, u], sems.at[XRR, u], right),
            remote(block.at[RIGHT, high], block.at[FAR, high], sems.at[XLS, u], sems.at[XLR, u], left),
        )

    def flat(ref_value):
        count, cap, lanes = ref_value.shape
        return ref_value.astype(F32).reshape(count * cap, lanes).astype(BF16)

    def arrive(u):
        batch = u // plain
        spread_wait(sbuf.at[u], rbuf.at[u], sems.at[PS, u], sems.at[PR, u], batch, True)

        @pl.when(batch == 0)
        def _():
            rbuf[u, 0] = sbuf[u, 0]

        xbuf[u, OWN] = flat(rbuf[u])
        for copy in y_send(xbuf.at[u], u):
            copy.start()

    def pass_on(block, u):
        for copy in y_send(block, u):
            copy.wait_recv()
        for copy in y_relay(block, u):
            copy.start()

    def multiply(u):
        for copy in y_relay(xbuf.at[u], u):
            copy.wait_recv()
        batch = u // plain
        add_chunk(xbuf[u].reshape(nodes * rows, width), batch, u - batch * plain + 1)

    def add_chunk(x, batch, c):
        at = pl.ds(pl.multiple_of(c * width, width), width)
        for e in range(EXP_DEV):
            acc[batch, 2 * e] += dot(x, wg[e, at, :])
            acc[batch, 2 * e + 1] += dot(x, wu[e, at, :])

    def z_piece(batch):
        return zbuf.at[:, pl.ds(batch * some, some)], steps + 1 + batch

    def spread_planes(src, dst, send, recv, batch):
        def one(j, carry):
            peer = plane_peer(BATCHES * j + batch)
            here, there = batch * some + j, batch * some + some - batch - j
            remote(src.at[:, here], dst.at[:, there], send, recv, peer).start()
            return carry

        lax.fori_loop(1 - batch, some, one, 0)

    def planes_desc(src, dst, send, recv, batch):
        at = pl.ds(batch * some + 1 - batch, some - 1 + batch)
        return remote(src.at[:, at], dst.at[:, at], send, recv, plane_peer(1))

    def z_plane(batch):
        u = steps + 1 + batch
        return zbuf, zin, sems.at[PS, u], sems.at[PR, u], batch

    def w_plane(batch):
        u = steps + 1 + batch
        return wbuf, win, sems.at[RS, u], sems.at[RR, u], batch

    def z_out(batch):
        for copy in y_relay(*z_piece(batch)):
            copy.wait_recv()
        spread_planes(*z_plane(batch))

    def z_multiply(batch):
        planes_desc(*z_plane(batch)).wait_recv()
        if batch == 0:
            zin[:, 0] = zbuf[:, 0]
        x = zin[:, batch * some : (batch + 1) * some].astype(F32)
        add_chunk(x.reshape(nodes * rows, width).astype(BF16), batch, 0)

    def w_project(batch):
        if batch == 0:
            wd_copy(plain).wait()
        part = dot(hid[batch], wd[plain])
        wbuf[:, batch * some : (batch + 1) * some] = part.reshape(nodes, some, CAP, width).astype(BF16)
        spread_planes(*w_plane(batch))

    def w_far(batch):
        u, mid = steps + 1 + batch, some // 2
        first, second = pl.ds(batch * some, mid), pl.ds(batch * some + mid, mid)
        return (
            remote(win.at[FAR, first], far_r.at[batch], sems.at[ORS, u], sems.at[ORR, u], right),
            remote(win.at[FAR, second], far_l.at[batch], sems.at[OLS, u], sems.at[OLR, u], left),
        )

    def w_near(batch):
        u = steps + 1 + batch
        return (
            remote(wnr.at[batch], wnr_in.at[batch], sems.at[NRS, u], sems.at[NRR, u], right),
            remote(wnl.at[batch], wnl_in.at[batch], sems.at[NLS, u], sems.at[NLR, u], left),
        )

    def w_opposite(batch):
        planes_desc(*w_plane(batch)).wait_recv()
        if batch == 0:
            win[:, 0] = wbuf[:, 0]
        for copy in w_far(batch):
            copy.start()

    def w_neighbour(batch):
        low, mid, high = batch * some, batch * some + some // 2, (batch + 1) * some
        for copy in w_far(batch):
            copy.wait_recv()
        wnr[batch, : some // 2] = (
            win[RIGHT, low:mid].astype(F32) + far_r[batch].astype(F32)
        ).astype(BF16)
        wnr[batch, some // 2 :] = win[RIGHT, mid:high]
        wnl[batch, : some // 2] = win[LEFT, low:mid]
        wnl[batch, some // 2 :] = (
            win[LEFT, mid:high].astype(F32) + far_l[batch].astype(F32)
        ).astype(BF16)
        for copy in w_near(batch):
            copy.start()

    def w_finish(batch):
        for copy in w_near(batch):
            copy.wait_recv()
        part = win[OWN, batch * some : (batch + 1) * some].astype(F32)
        part = part + wnr_in[batch].astype(F32) + wnl_in[batch].astype(F32)
        return dot(
            place_t_ref[:, batch * rows : (batch + 1) * rows], part.reshape(rows, width).astype(BF16)
        )

    def activate(batch):
        w_all = wx[:, pl.ds(pl.multiple_of(batch * rows, rows), rows), :]
        w_all = w_all.astype(F32).reshape(nodes * rows, LANES)
        for e in range(EXP_DEV):
            gate = acc[batch, 2 * e]
            gain = jnp.broadcast_to(w_all[:, e * (LANES // 2) : e * (LANES // 2) + 1], gate.shape)
            value = gate / (1.0 + jnp.exp(-gate)) * acc[batch, 2 * e + 1] * gain
            hid[batch, :, e * ff : (e + 1) * ff] = value.astype(BF16)

    def opposite(u):
        return (
            remote(opr.at[u], opr_in.at[u], sems.at[ORS, u], sems.at[ORR, u], right),
            remote(opl.at[u], opl_in.at[u], sems.at[OLS, u], sems.at[OLR, u], left),
        )

    def neighbour(u):
        return (
            remote(nbr.at[u], nbr_in.at[u], sems.at[NRS, u], sems.at[NRR, u], right),
            remote(nbl.at[u], nbl_in.at[u], sems.at[NLS, u], sems.at[NLR, u], left),
        )

    def project(u, first, count):
        batch = u // plain
        return dot(hid[batch, first * rows : (first + count) * rows, :], wd[u - batch * plain])

    def start_opposite(u):
        @pl.when(u < plain)
        def _():
            wd_copy(u).wait()

        part = project(u, FAR, 1)
        opr[u] = part[:half].astype(BF16)
        opl[u] = part[half:].astype(BF16)
        for copy in opposite(u):
            copy.start()

    def start_neighbour(u):
        part = project(u, RIGHT, 2)
        for copy in opposite(u):
            copy.wait_recv()
        nbr[u, :half] = (part[:half] + opr_in[u].astype(F32)).astype(BF16)
        nbr[u, half:] = part[half:rows].astype(BF16)
        nbl[u, :half] = part[rows : rows + half].astype(BF16)
        nbl[u, half:] = (part[rows + half :] + opl_in[u].astype(F32)).astype(BF16)
        for copy in neighbour(u):
            copy.start()

    def finish(u):
        part = project(u, OWN, 1)
        for copy in neighbour(u):
            copy.wait_recv()
        part = part + nbr_in[u].astype(F32) + nbl_in[u].astype(F32)
        rsb[u] = part.reshape(some, CAP, width).astype(BF16)
        spread(rsb.at[u], rrb.at[u], sems.at[RS, u], sems.at[RR, u], u // plain)

    def collect(c):
        total = jnp.zeros((rows_tok, width), F32)
        for b in range(BATCHES):
            u = b * plain + c
            spread_desc(
                rsb.at[u], rrb.at[u], sems.at[RS, u], sems.at[RR, u], 1 - b, some
            ).wait_recv()
            if b == 0:
                rrb[u, 0] = rsb[u, 0]
            total += dot(place_t_ref[:, b * rows : (b + 1) * rows], flat(rrb[u]))
        out_ref[:, pl.ds(pl.multiple_of(c * width, width), width)] = total.astype(BF16)

    prepare(0)
    pl.semaphore_wait(barrier, len(greeted))
    for b in range(BATCHES):
        for copy in y_send(*z_piece(b)):
            copy.start()
    acc[...] = jnp.zeros_like(acc)
    for device in beside:
        pl.semaphore_signal(round_sem, inc=1, device_id=device, device_id_type=MESH)
    prepare(1)
    pl.semaphore_wait(round_sem, len(beside))
    for c in range(2, chunks):
        if c - 2 < EARLY:
            send_plane(c - 2)
        prepare(c)
        if c == 4:
            pass_on(*z_piece(0))
    for b in range(BATCHES):
        at = pl.ds(b * some, some)
        spread(wsb.at[at], wrb.at[at], sems.at[PS, steps], sems.at[PR, steps], b)
    pass_on(*z_piece(1))

    lag_y, lag_x, lag_m = 0, 2, 4
    lag_o = steps + 1
    lag_n, lag_f, lag_c = lag_o + 2, lag_o + 4, lag_o + 6

    def stage(s, lag, first, last, work):
        @pl.when((s >= lag + first) & (s < lag + last))
        def _():
            work(s - lag)

    def at_step(s, step, work, *args):
        @pl.when(s == step)
        def _():
            work(*args)

    def share_weights():
        spread_desc(wsb, wrb, sems.at[PS, steps], sems.at[PR, steps], 1, groups).wait_recv()
        wrb[0] = wsb[0]
        wx[OWN] = flat(wrb[...])
        for copy in y_send(wx, steps):
            copy.start()

    def have_gate_up():
        wg_copy.wait()
        wu_copy.wait()

    def have_weights():
        for copy in y_relay(wx, steps):
            copy.wait_recv()

    def turn(batch):
        z_multiply(batch)
        activate(batch)
        w_project(batch)

    def w_last():
        total = w_finish(0) + w_finish(1)
        out_ref[:, plain * width :] = total.astype(BF16)

    def send_two(k):
        send_plane(EARLY + 2 * k)
        send_plane(EARLY + 1 + 2 * k)

    def whole(s, carry):
        stage(s, 0, 0, (steps - EARLY) // 2, send_two)
        stage(s, lag_y, 0, steps, arrive)
        at_step(s, 3, share_weights)
        at_step(s, 3, have_gate_up)
        stage(s, lag_x, 0, steps, lambda u: pass_on(xbuf.at[u], u))
        at_step(s, 5, pass_on, wx, steps)
        at_step(s, 4, z_out, 0)
        at_step(s, 5, z_out, 1)
        stage(s, lag_m, 0, steps, multiply)
        at_step(s, 8, have_weights)
        at_step(s, steps, turn, 0)
        at_step(s, lag_m + steps - 1, turn, 1)
        stage(s, lag_o, 0, steps, start_opposite)
        at_step(s, lag_o + steps, w_opposite, 0)
        at_step(s, lag_o + steps + 1, w_opposite, 1)
        stage(s, lag_n, 0, steps, start_neighbour)
        at_step(s, lag_n + steps, w_neighbour, 0)
        at_step(s, lag_n + steps + 1, w_neighbour, 1)
        stage(s, lag_f, 0, steps, finish)
        stage(s, lag_c + steps - plain, 0, plain, collect)
        at_step(s, lag_f + steps + 1, w_last)
        return carry

    lax.fori_loop(0, lag_f + steps + 2, whole, 0)

    def drain(u, carry):
        spread_wait(sbuf.at[u], rbuf.at[u], sems.at[PS, u], sems.at[PR, u], u // plain, False)
        spread_wait(rsb.at[u], rrb.at[u], sems.at[RS, u], sems.at[RR, u], u // plain, False)
        for copy in y_send(xbuf.at[u], u) + y_relay(xbuf.at[u], u) + opposite(u) + neighbour(u):
            copy.wait_send()

        return carry

    lax.fori_loop(0, steps, drain, 0)
    spread_desc(wsb, wrb, sems.at[PS, steps], sems.at[PR, steps], 1, groups).wait_send()
    for copy in y_send(wx, steps) + y_relay(wx, steps):
        copy.wait_send()
    for b in range(BATCHES):
        planes_desc(*z_plane(b)).wait_send()
        planes_desc(*w_plane(b)).wait_send()
        for copy in y_send(*z_piece(b)) + y_relay(*z_piece(b)) + w_far(b) + w_near(b):
            copy.wait_send()


def solution(mesh):
    nodes, groups = mesh.shape["node"], mesh.shape["torus"]

    def shards(tokens, expert_ids, route_weight, w_gate, w_up, w_down):
        rows_tok, depth = tokens.shape
        ff = w_gate.shape[2]
        width = min(CHUNK, depth)
        chunks = depth // width
        slots = groups * CAP
        steps = BATCHES * (chunks - 1)
        some = groups // BATCHES
        rows = some * CAP
        anywhere = pl.BlockSpec(memory_space=pl.ANY)
        inside = pl.BlockSpec(memory_space=pltpu.VMEM)
        block = pltpu.VMEM((steps, some, CAP, width), BF16)
        planes = pltpu.VMEM((nodes, groups, CAP, width), BF16)
        piece = pltpu.VMEM((BATCHES, some, CAP, width), BF16)
        halves = pltpu.VMEM((steps, rows // 2, width), BF16)
        whole = pltpu.VMEM((steps, rows, width), BF16)
        return pl.pallas_call(
            functools.partial(layer, nodes, groups),
            out_shape=pltpu.VMEM((rows_tok, depth), BF16),
            in_specs=[anywhere, inside, inside, anywhere, anywhere, anywhere],
            out_specs=inside,
            scratch_shapes=[
                pltpu.VMEM((chunks, rows_tok, width), BF16),
                pltpu.VMEM(w_gate.shape, BF16),
                pltpu.VMEM(w_up.shape, BF16),
                pltpu.VMEM((chunks, EXP_DEV * ff, width), BF16),
                block,
                block,
                pltpu.VMEM((steps, nodes, rows, width), BF16),
                pltpu.VMEM((groups, CAP, LANES), BF16),
                pltpu.VMEM((groups, CAP, LANES), BF16),
                pltpu.VMEM((nodes, slots, LANES), BF16),
                pltpu.VMEM((BATCHES, 2 * EXP_DEV, nodes * rows, ff), F32),
                pltpu.VMEM((BATCHES, nodes * rows, EXP_DEV * ff), BF16),
                halves,
                halves,
                halves,
                halves,
                whole,
                whole,
                whole,
                whole,
                block,
                block,
                planes,
                planes,
                planes,
                planes,
                pltpu.VMEM((BATCHES, some // 2, CAP, width), BF16),
                pltpu.VMEM((BATCHES, some // 2, CAP, width), BF16),
                piece,
                piece,
                piece,
                piece,
                pltpu.VMEM((slots, rows_tok), BF16),
                pltpu.VMEM((rows_tok, slots), BF16),
                pltpu.SemaphoreType.DMA((N_SEMS, steps + 1 + BATCHES)),
                pltpu.SemaphoreType.REGULAR,
            ],
            compiler_params=pltpu.CompilerParams(
                collective_id=0, has_side_effects=True, vmem_limit_bytes=58500000
            ),
        )(
            tokens,
            expert_ids.T,
            route_weight.T,
            w_gate,
            w_up,
            w_down.reshape(EXP_DEV * ff, depth),
        )

    placed = (
        P(("node", "torus"), None),
        P(("node", "torus"), None),
        P(("node", "torus"), None),
        P("torus", None, "node"),
        P("torus", None, "node"),
        P("torus", "node", None),
    )
    return jax.shard_map(
        shards, mesh=mesh, in_specs=placed, out_specs=P(("node", "torus"), None), check_vma=False
    )
```

```python
import functools

import jax
import jax.numpy as jnp
from jax import lax
from jax.experimental import pallas as pl
from jax.experimental.pallas import tpu as pltpu
from jax.sharding import PartitionSpec as P

EXP_DEV = 2
CAP = 4
QBLOCK = 128
LANES = 128
CHUNK = 1024
BATCHES = 2
EARLY = 4
PACK = 16
MESH = pl.DeviceIdType.MESH
F32 = jnp.float32
BF16 = jnp.bfloat16

TOK, PS, PR, YRS, YRR, YLS, YLR, XRS, XRR, XLS, XLR = range(11)
ORS, ORR, OLS, OLR, NRS, NRR, NLS, NLR, RS, RR, WT, OUT = range(11, 23)
N_SEMS = 23


def dot(a, b):
    return jnp.dot(a, b, preferred_element_type=F32)


def layer(
    nodes,
    groups,
    tok_hbm,
    ids_hbm,
    rw_hbm,
    wg_hbm,
    wu_hbm,
    wd_hbm,
    out_ref,
    ids_ref,
    rw_ref,
    tok,
    wg,
    wu,
    wd,
    sbuf,
    rbuf,
    xbuf,
    wsb,
    wrb,
    wx,
    wcol,
    acc,
    hid,
    opr,
    opl,
    opr_in,
    opl_in,
    nbr,
    nbl,
    nbr_in,
    nbl_in,
    rsb,
    rrb,
    zbuf,
    zin,
    wbuf,
    win,
    far_r,
    far_l,
    wnr,
    wnl,
    wnr_in,
    wnl_in,
    place_ref,
    place_t_ref,
    sems,
    round_sem,
):
    chunks, rows_tok, width = tok.shape
    plain = chunks - 1
    steps = BATCHES * plain
    some = groups // BATCHES
    slots = groups * CAP
    rows = some * CAP
    half = rows // 2
    ff = wg.shape[2]
    me_n = lax.axis_index("node")
    me_t = lax.axis_index("torus")
    right = (lax.rem(me_n + 1, nodes), me_t)
    left = (lax.rem(me_n + nodes - 1, nodes), me_t)
    OWN, RIGHT, LEFT, FAR = range(4)

    def plane_peer(r):
        return (me_n, lax.rem(me_t + r, groups))

    def remote(src, dst, send, recv, device):
        return pltpu.make_async_remote_copy(
            src_ref=src,
            dst_ref=dst,
            send_sem=send,
            recv_sem=recv,
            device_id=device,
            device_id_type=MESH,
        )

    def spread(src, dst, send, recv, batch):
        def one(j, carry):
            peer = plane_peer(BATCHES * j + batch)
            remote(src.at[j], dst.at[some - batch - j], send, recv, peer).start()
            return carry

        lax.fori_loop(1 - batch, some, one, 0)

    def spread_desc(src, dst, send, recv, low, high):
        at = pl.ds(low, high - low)
        return remote(src.at[at], dst.at[at], send, recv, plane_peer(1))

    def spread_wait(src, dst, send, recv, batch, received):
        for b in range(BATCHES):

            @pl.when(batch == b)
            def _(b=b):
                copy = spread_desc(src, dst, send, recv, 1 - b, some)
                if received:
                    copy.wait_recv()
                else:
                    copy.wait_send()

    across = min(4, groups // 2)
    deep = groups // (2 * across)
    me_core, me_x, me_z = lax.rem(me_t, 2), lax.rem(me_t // 2, across), me_t // (2 * across)

    def torus_peer(dz, dx, dc):
        z, x, core = lax.rem(me_z + dz, deep), lax.rem(me_x + dx, across), lax.rem(me_core + dc, 2)
        return (me_n, (z * across + x) * 2 + core)

    beside = [torus_peer(0, dx, 0) for dx in range(1, across)]
    greeted = [right, left, torus_peer(0, 0, 1)] + beside
    greeted += [torus_peer(0, dx, 1) for dx in range(1, across)]
    greeted += [torus_peer(dz, 0, dc) for dz in range(1, deep) for dc in range(2)]
    barrier = pltpu.get_barrier_semaphore()
    for device in greeted:
        pl.semaphore_signal(barrier, inc=1, device_id=device, device_id_type=MESH)

    def tok_copy(c):
        return pltpu.make_async_copy(
            tok_hbm.at[:, pl.ds(pl.multiple_of(c * width, width), width)],
            tok.at[c],
            sems.at[TOK, c],
        )

    def wd_copy(c):
        return pltpu.make_async_copy(
            wd_hbm.at[:, pl.ds(pl.multiple_of(c * width, width), width)],
            wd.at[c],
            sems.at[WT, c],
        )

    wg_copy = pltpu.make_async_copy(wg_hbm, wg, sems.at[TOK, chunks])
    wu_copy = pltpu.make_async_copy(wu_hbm, wu, sems.at[WT, chunks])
    ids_copy = pltpu.make_async_copy(ids_hbm, ids_ref, sems.at[OUT, 0])
    rw_copy = pltpu.make_async_copy(rw_hbm, rw_ref, sems.at[OUT, 1])
    ids_copy.start()
    rw_copy.start()
    for c in range(chunks):
        tok_copy(c).start()
    wg_copy.start()
    wu_copy.start()
    for c in range(chunks):
        wd_copy(c).start()

    slot = lax.broadcasted_iota(jnp.int32, (slots, rows_tok), 0)
    spot = slot // CAP
    offset = BATCHES * lax.rem(spot, some) + spot // some
    group = lax.rem(me_t + offset, groups)
    ids_copy.wait()
    rw_copy.wait()
    ids = ids_ref[...]
    weights = rw_ref[...].astype(F32)
    member = jnp.zeros((slots, rows_tok), F32)
    weight_a = jnp.zeros((slots, rows_tok), F32)
    weight_b = jnp.zeros((slots, rows_tok), F32)
    for k in range(ids.shape[0]):
        one = jnp.broadcast_to(ids[k : k + 1, :], (slots, rows_tok))
        gain = jnp.broadcast_to(weights[k : k + 1, :], (slots, rows_tok))
        is_a = one == 2 * group
        is_b = one == 2 * group + 1
        weight_a = jnp.where(is_a, gain, weight_a)
        weight_b = jnp.where(is_b, gain, weight_b)
        member = jnp.where(is_a | is_b, jnp.float32(1.0), member)
    before = (
        lax.broadcasted_iota(jnp.int32, (rows_tok, rows_tok), 0)
        < lax.broadcasted_iota(jnp.int32, (rows_tok, rows_tok), 1)
    )
    before = jnp.where(before, jnp.float32(1.0), jnp.float32(0.0)).astype(BF16)
    index = dot(member.astype(BF16), before)
    here = index == lax.rem(slot, CAP).astype(F32)
    place = jnp.where(here, member, jnp.float32(0.0))
    place_ref[...] = place.astype(BF16)
    place_t_ref[...] = jnp.transpose(place).astype(BF16)
    lane = lax.broadcasted_iota(jnp.int32, (rows_tok, LANES), 1)
    low = jnp.where(lane < LANES // 2, jnp.float32(1.0), jnp.float32(0.0))
    spread_w = dot((place * weight_a).astype(BF16), low.astype(BF16)) + dot(
        (place * weight_b).astype(BF16), (1.0 - low).astype(BF16)
    )
    wsb[...] = spread_w.reshape(groups, CAP, LANES).astype(BF16)

    def prepare(c):
        tok_copy(c).wait()
        parts = []
        for b in range(width // QBLOCK):
            x = tok[c, :, b * QBLOCK : (b + 1) * QBLOCK].astype(F32)
            top = jnp.max(jnp.abs(x), axis=1, keepdims=True)
            scale = ((top + 1e-06) * (1.0 / 448.0)).astype(BF16).astype(F32)
            scale = jnp.broadcast_to(scale, x.shape)
            quantized = (x / scale).astype(BF16)
            parts.append((quantized.astype(F32) * scale).astype(BF16))
        restored = jnp.concatenate(parts, axis=1)
        picked = dot(place_ref[...], restored).reshape(groups, CAP, width).astype(BF16)
        if c == 0:
            zbuf[OWN] = picked
        else:
            for b in range(BATCHES):
                sbuf[b * plain + c - 1] = picked[b * some : (b + 1) * some]

    def send_plane(u):
        spread(sbuf.at[u], rbuf.at[u], sems.at[PS, u], sems.at[PR, u], u // plain)

    def y_send(block, u):
        return (
            remote(block.at[OWN], block.at[LEFT], sems.at[YRS, u], sems.at[YRR, u], right),
            remote(block.at[OWN], block.at[RIGHT], sems.at[YLS, u], sems.at[YLR, u], left),
        )

    def y_relay(block, u):
        middle = block.shape[1] // 2
        low, high = pl.ds(0, middle), pl.ds(middle, middle)
        return (
            remote(block.at[LEFT, low], block.at[FAR, low], sems.at[XRS, u], sems.at[XRR, u], right),
            remote(block.at[RIGHT, high], block.at[FAR, high], sems.at[XLS, u], sems.at[XLR, u], left),
        )

    def flat(ref_value):
        count, cap, lanes = ref_value.shape
        return ref_value.astype(F32).reshape(count * cap, lanes).astype(BF16)

    def arrive(u):
        batch = u // plain
        spread_wait(sbuf.at[u], rbuf.at[u], sems.at[PS, u], sems.at[PR, u], batch, True)

        @pl.when(batch == 0)
        def _():
            rbuf[u, 0] = sbuf[u, 0]

        xbuf[u, OWN] = flat(rbuf[u])
        for copy in y_send(xbuf.at[u], u):
            copy.start()

    def pass_on(block, u):
        for copy in y_send(block, u):
            copy.wait_recv()
        for copy in y_relay(block, u):
            copy.start()

    def multiply(u):
        for copy in y_relay(xbuf.at[u], u):
            copy.wait_recv()
        batch = u // plain
        add_chunk(xbuf[u].reshape(nodes * rows, width), batch, u - batch * plain + 1)

    def add_chunk(x, batch, c):
        at = pl.ds(pl.multiple_of(c * width, width), width)
        for e in range(EXP_DEV):
            acc[batch, 2 * e] += dot(x, wg[e, at, :])
            acc[batch, 2 * e + 1] += dot(x, wu[e, at, :])

    def z_piece(batch):
        return zbuf.at[:, pl.ds(batch * some, some)], steps + 1 + batch

    def spread_planes(src, dst, send, recv, batch):
        def one(j, carry):
            peer = plane_peer(BATCHES * j + batch)
            here, there = batch * some + j, batch * some + some - batch - j
            remote(src.at[:, here], dst.at[:, there], send, recv, peer).start()
            return carry

        lax.fori_loop(1 - batch, some, one, 0)

    def planes_desc(src, dst, send, recv, batch):
        at = pl.ds(batch * some + 1 - batch, some - 1 + batch)
        return remote(src.at[:, at], dst.at[:, at], send, recv, plane_peer(1))

    def z_plane(batch):
        u = steps + 1 + batch
        return zbuf, zin, sems.at[PS, u], sems.at[PR, u], batch

    def w_plane(batch):
        u = steps + 1 + batch
        return wbuf, win, sems.at[RS, u], sems.at[RR, u], batch

    def z_out(batch):
        for copy in y_relay(*z_piece(batch)):
            copy.wait_recv()
        spread_planes(*z_plane(batch))

    def z_multiply(batch):
        planes_desc(*z_plane(batch)).wait_recv()
        if batch == 0:
            zin[:, 0] = zbuf[:, 0]
        x = zin[:, batch * some : (batch + 1) * some].astype(F32)
        add_chunk(x.reshape(nodes * rows, width).astype(BF16), batch, 0)

    def w_project(batch):
        if batch == 0:
            wd_copy(plain).wait()
        part = dot(hid[batch], wd[plain])
        wbuf[:, batch * some : (batch + 1) * some] = part.reshape(nodes, some, CAP, width).astype(BF16)
        spread_planes(*w_plane(batch))

    def w_far(batch):
        u, mid = steps + 1 + batch, some // 2
        first, second = pl.ds(batch * some, mid), pl.ds(batch * some + mid, mid)
        return (
            remote(win.at[FAR, first], far_r.at[batch], sems.at[ORS, u], sems.at[ORR, u], right),
            remote(win.at[FAR, second], far_l.at[batch], sems.at[OLS, u], sems.at[OLR, u], left),
        )

    def w_near(batch):
        u = steps + 1 + batch
        return (
            remote(wnr.at[batch], wnr_in.at[batch], sems.at[NRS, u], sems.at[NRR, u], right),
            remote(wnl.at[batch], wnl_in.at[batch], sems.at[NLS, u], sems.at[NLR, u], left),
        )

    def w_opposite(batch):
        planes_desc(*w_plane(batch)).wait_recv()
        if batch == 0:
            win[:, 0] = wbuf[:, 0]
        for copy in w_far(batch):
            copy.start()

    def w_neighbour(batch):
        low, mid, high = batch * some, batch * some + some // 2, (batch + 1) * some
        for copy in w_far(batch):
            copy.wait_recv()
        wnr[batch, : some // 2] = (
            win[RIGHT, low:mid].astype(F32) + far_r[batch].astype(F32)
        ).astype(BF16)
        wnr[batch, some // 2 :] = win[RIGHT, mid:high]
        wnl[batch, : some // 2] = win[LEFT, low:mid]
        wnl[batch, some // 2 :] = (
            win[LEFT, mid:high].astype(F32) + far_l[batch].astype(F32)
        ).astype(BF16)
        for copy in w_near(batch):
            copy.start()

    def w_finish(batch):
        for copy in w_near(batch):
            copy.wait_recv()
        part = win[OWN, batch * some : (batch + 1) * some].astype(F32)
        part = part + wnr_in[batch].astype(F32) + wnl_in[batch].astype(F32)
        return dot(
            place_t_ref[:, batch * rows : (batch + 1) * rows], part.reshape(rows, width).astype(BF16)
        )

    def activate(batch):
        for e in range(EXP_DEV):
            gate = acc[batch, 2 * e]
            gain = wcol[e, :, batch * rows : (batch + 1) * rows, :].reshape(nodes * rows, LANES)
            gain = jnp.broadcast_to(gain[:, :1], gate.shape)
            value = gate / (1.0 + jnp.exp(-gate)) * acc[batch, 2 * e + 1] * gain
            hid[batch, :, e * ff : (e + 1) * ff] = value.astype(BF16)

    def opposite(u):
        return (
            remote(opr.at[u], opr_in.at[u], sems.at[ORS, u], sems.at[ORR, u], right),
            remote(opl.at[u], opl_in.at[u], sems.at[OLS, u], sems.at[OLR, u], left),
        )

    def neighbour(u):
        return (
            remote(nbr.at[u], nbr_in.at[u], sems.at[NRS, u], sems.at[NRR, u], right),
            remote(nbl.at[u], nbl_in.at[u], sems.at[NLS, u], sems.at[NLR, u], left),
        )

    def project(u, first, count):
        batch = u // plain
        return dot(hid[batch, first * rows : (first + count) * rows, :], wd[u - batch * plain])

    def start_opposite(u):
        @pl.when(u < plain)
        def _():
            wd_copy(u).wait()

        part = project(u, FAR, 1)
        opr[u] = part[:half].astype(BF16)
        opl[u] = part[half:].astype(BF16)
        for copy in opposite(u):
            copy.start()

    def start_neighbour(u):
        part = project(u, RIGHT, 2)
        for copy in opposite(u):
            copy.wait_recv()
        nbr[u, :half] = (part[:half] + opr_in[u].astype(F32)).astype(BF16)
        nbr[u, half:] = part[half:rows].astype(BF16)
        nbl[u, :half] = part[rows : rows + half].astype(BF16)
        nbl[u, half:] = (part[rows + half :] + opl_in[u].astype(F32)).astype(BF16)
        for copy in neighbour(u):
            copy.start()

    def finish(u):
        part = project(u, OWN, 1)
        for copy in neighbour(u):
            copy.wait_recv()
        part = part + nbr_in[u].astype(F32) + nbl_in[u].astype(F32)
        rsb[u] = part.reshape(some, CAP, width).astype(BF16)
        spread(rsb.at[u], rrb.at[u], sems.at[RS, u], sems.at[RR, u], u // plain)

    def collect(c):
        total = jnp.zeros((rows_tok, width), F32)
        for b in range(BATCHES):
            u = b * plain + c
            spread_desc(
                rsb.at[u], rrb.at[u], sems.at[RS, u], sems.at[RR, u], 1 - b, some
            ).wait_recv()
            if b == 0:
                rrb[u, 0] = rsb[u, 0]
            total += dot(place_t_ref[:, b * rows : (b + 1) * rows], flat(rrb[u]))
        out_ref[:, pl.ds(pl.multiple_of(c * width, width), width)] = total.astype(BF16)

    prepare(0)
    pl.semaphore_wait(barrier, len(greeted))
    for b in range(BATCHES):
        for copy in y_send(*z_piece(b)):
            copy.start()
    acc[...] = jnp.zeros_like(acc)
    for device in beside:
        pl.semaphore_signal(round_sem, inc=1, device_id=device, device_id_type=MESH)
    prepare(1)
    pl.semaphore_wait(round_sem, len(beside))
    for c in range(2, chunks):
        if c - 2 < EARLY:
            send_plane(c - 2)
        prepare(c)
        if c == 4:
            pass_on(*z_piece(0))
    for b in range(BATCHES):
        at = pl.ds(b * some, some)
        spread(wsb.at[at], wrb.at[at], sems.at[PS, steps], sems.at[PR, steps], b)
    arrive(0)
    pass_on(*z_piece(1))

    lag_y, lag_x, lag_m = 0, 2, 4
    lag_o = steps + 1
    lag_n, lag_f, lag_c = lag_o + 2, lag_o + 4, lag_o + 6

    def stage(s, lag, first, last, work):
        @pl.when((s >= lag + first) & (s < lag + last))
        def _():
            work(s - lag)

    def at_step(s, step, work, *args):
        @pl.when(s == step)
        def _():
            work(*args)

    def share_weights():
        spread_desc(wsb, wrb, sems.at[PS, steps], sems.at[PR, steps], 1, groups).wait_recv()
        wrb[0] = wsb[0]
        turned = jnp.transpose(wrb[...].astype(F32).reshape(slots, LANES)).astype(BF16)
        for e in range(EXP_DEV):
            first = e * (LANES // EXP_DEV)
            wx[OWN, e * PACK : (e + 1) * PACK] = turned[first : first + PACK]
        for copy in y_send(wx, steps):
            copy.start()

    def have_gate_up():
        wg_copy.wait()
        wu_copy.wait()

    def have_weights():
        for copy in y_relay(wx, steps):
            copy.wait_recv()
        for e in range(EXP_DEV):
            for plane in range(nodes):
                line = wx[plane, e * PACK : e * PACK + 1, :].astype(F32)
                wcol[e, plane] = jnp.transpose(jnp.broadcast_to(line, (LANES, slots)))

    def turn(batch):
        z_multiply(batch)
        activate(batch)
        w_project(batch)

    def w_last():
        total = w_finish(0) + w_finish(1)
        out_ref[:, plain * width :] = total.astype(BF16)

    def send_two(k):
        send_plane(EARLY + 2 * k)
        send_plane(EARLY + 1 + 2 * k)

    def whole(s, carry):
        stage(s, 0, 0, (steps - EARLY) // 2, send_two)
        stage(s, lag_y, 1, steps, arrive)
        at_step(s, 3, share_weights)
        at_step(s, 3, have_gate_up)
        stage(s, lag_x, 0, steps, lambda u: pass_on(xbuf.at[u], u))
        at_step(s, 5, pass_on, wx, steps)
        at_step(s, 4, z_out, 0)
        at_step(s, 5, z_out, 1)
        stage(s, lag_m, 0, steps, multiply)
        at_step(s, 8, have_weights)
        at_step(s, steps, turn, 0)
        at_step(s, lag_m + steps - 1, turn, 1)
        stage(s, lag_o, 0, steps, start_opposite)
        at_step(s, lag_o + steps, w_opposite, 0)
        at_step(s, lag_o + steps + 1, w_opposite, 1)
        stage(s, lag_n, 0, steps, start_neighbour)
        at_step(s, lag_n + steps, w_neighbour, 0)
        at_step(s, lag_n + steps + 1, w_neighbour, 1)
        stage(s, lag_f, 0, steps, finish)
        stage(s, lag_c + steps - plain, 0, plain, collect)
        at_step(s, lag_f + steps + 1, w_last)
        return carry

    lax.fori_loop(0, lag_f + steps + 2, whole, 0)

    def drain(u, carry):
        spread_wait(sbuf.at[u], rbuf.at[u], sems.at[PS, u], sems.at[PR, u], u // plain, False)
        spread_wait(rsb.at[u], rrb.at[u], sems.at[RS, u], sems.at[RR, u], u // plain, False)
        for copy in y_send(xbuf.at[u], u) + y_relay(xbuf.at[u], u) + opposite(u) + neighbour(u):
            copy.wait_send()

        return carry

    lax.fori_loop(0, steps, drain, 0)
    spread_desc(wsb, wrb, sems.at[PS, steps], sems.at[PR, steps], 1, groups).wait_send()
    for copy in y_send(wx, steps) + y_relay(wx, steps):
        copy.wait_send()
    for b in range(BATCHES):
        planes_desc(*z_plane(b)).wait_send()
        planes_desc(*w_plane(b)).wait_send()
        for copy in y_send(*z_piece(b)) + y_relay(*z_piece(b)) + w_far(b) + w_near(b):
            copy.wait_send()


def solution(mesh):
    nodes, groups = mesh.shape["node"], mesh.shape["torus"]

    def shards(tokens, expert_ids, route_weight, w_gate, w_up, w_down):
        rows_tok, depth = tokens.shape
        ff = w_gate.shape[2]
        width = min(CHUNK, depth)
        chunks = depth // width
        slots = groups * CAP
        steps = BATCHES * (chunks - 1)
        some = groups // BATCHES
        rows = some * CAP
        anywhere = pl.BlockSpec(memory_space=pl.ANY)
        inside = pl.BlockSpec(memory_space=pltpu.VMEM)
        block = pltpu.VMEM((steps, some, CAP, width), BF16)
        planes = pltpu.VMEM((nodes, groups, CAP, width), BF16)
        piece = pltpu.VMEM((BATCHES, some, CAP, width), BF16)
        halves = pltpu.VMEM((steps, rows // 2, width), BF16)
        whole = pltpu.VMEM((steps, rows, width), BF16)
        return pl.pallas_call(
            functools.partial(layer, nodes, groups),
            out_shape=pltpu.VMEM((rows_tok, depth), BF16),
            in_specs=[anywhere] * 6,
            out_specs=inside,
            scratch_shapes=[
                pltpu.VMEM(expert_ids.shape[::-1], jnp.int32),
                pltpu.VMEM(route_weight.shape[::-1], BF16),
                pltpu.VMEM((chunks, rows_tok, width), BF16),
                pltpu.VMEM(w_gate.shape, BF16),
                pltpu.VMEM(w_up.shape, BF16),
                pltpu.VMEM((chunks, EXP_DEV * ff, width), BF16),
                block,
                block,
                pltpu.VMEM((steps, nodes, rows, width), BF16),
                pltpu.VMEM((groups, CAP, LANES), BF16),
                pltpu.VMEM((groups, CAP, LANES), BF16),
                pltpu.VMEM((nodes, EXP_DEV * PACK, slots), BF16),
                pltpu.VMEM((EXP_DEV, nodes, slots, LANES), F32),
                pltpu.VMEM((BATCHES, 2 * EXP_DEV, nodes * rows, ff), F32),
                pltpu.VMEM((BATCHES, nodes * rows, EXP_DEV * ff), BF16),
                halves,
                halves,
                halves,
                halves,
                whole,
                whole,
                whole,
                whole,
                block,
                block,
                planes,
                planes,
                planes,
                planes,
                pltpu.VMEM((BATCHES, some // 2, CAP, width), BF16),
                pltpu.VMEM((BATCHES, some // 2, CAP, width), BF16),
                piece,
                piece,
                piece,
                piece,
                pltpu.VMEM((slots, rows_tok), BF16),
                pltpu.VMEM((rows_tok, slots), BF16),
                pltpu.SemaphoreType.DMA((N_SEMS, steps + 1 + BATCHES)),
                pltpu.SemaphoreType.REGULAR,
            ],
            compiler_params=pltpu.CompilerParams(
                collective_id=0, has_side_effects=True, vmem_limit_bytes=59000000
            ),
        )(
            tokens,
            expert_ids.T,
            route_weight.T,
            w_gate,
            w_up,
            w_down.reshape(EXP_DEV * ff, depth),
        )

    placed = (
        P(("node", "torus"), None),
        P(("node", "torus"), None),
        P(("node", "torus"), None),
        P("torus", None, "node"),
        P("torus", None, "node"),
        P("torus", "node", None),
    )
    return jax.shard_map(
        shards, mesh=mesh, in_specs=placed, out_specs=P(("node", "torus"), None), check_vma=False
    )
```

```python
import functools

import jax
import jax.numpy as jnp
from jax import lax
from jax.experimental import pallas as pl
from jax.experimental.pallas import tpu as pltpu
from jax.sharding import PartitionSpec as P

EXP_DEV = 2
CAP = 4
QBLOCK = 128
LANES = 128
CHUNK = 1024
BATCHES = 2
EARLY = 4
PACK = 16
MESH = pl.DeviceIdType.MESH
F32 = jnp.float32
BF16 = jnp.bfloat16

(
    TOK_FIRST,
    TOK_REST,
    W_GATE,
    W_UP,
    W_DOWN,
    IDS,
    GAINS,
    PLANE_SENT,
    GAIN_PLANE_SENT,
    Z_PLANE_SENT,
    Y_SENT,
    RELAY_SENT,
    GAIN_Y_SENT,
    GAIN_RELAY_SENT,
    Z_Y_SENT,
    Z_RELAY_SENT,
    OPP_SENT,
    NEAR_SENT,
    BACK_SENT,
    W_FAR_SENT,
    W_NEAR_SENT,
    W_PLANE_SENT,
    PLANE_SENT_ODD,
    SINGLES,
) = range(24)


def dot(a, b):
    return jnp.dot(a, b, preferred_element_type=F32)


def layer(
    nodes,
    groups,
    tok_hbm,
    ids_hbm,
    rw_hbm,
    wg_hbm,
    wu_hbm,
    wd_hbm,
    out_ref,
    ids_ref,
    rw_ref,
    tok,
    wg,
    wu,
    wd,
    sbuf,
    rbuf,
    xbuf,
    wsb,
    wrb,
    wx,
    wcol,
    acc,
    hid,
    opp,
    opp_in,
    near,
    near_in,
    rsb,
    rrb,
    zbuf,
    zin,
    wbuf,
    win,
    w_opp_in,
    w_near,
    w_near_in,
    place_ref,
    place_t_ref,
    sems,
    round_sem,
):
    chunks, rows_tok, width = tok.shape
    plain = chunks - 1
    steps = BATCHES * plain
    some = groups // BATCHES
    slots = groups * CAP
    rows = some * CAP
    half = rows // 2
    ff = wg.shape[2]
    me_n = lax.axis_index("node")
    me_t = lax.axis_index("torus")
    right = (lax.rem(me_n + 1, nodes), me_t)
    left = (lax.rem(me_n + nodes - 1, nodes), me_t)
    OWN, RIGHT, LEFT, FAR = range(4)

    table = steps + 1 + BATCHES

    def plane_in(u):
        return sems.at[u]

    def near_sem(u):
        return sems.at[table + u]

    def far_sem(u):
        return sems.at[2 * table + u]

    def back_sem(c):
        return sems.at[3 * table + c]

    def single(k):
        return sems.at[3 * table + plain + BATCHES + k]

    def plane_peer(r):
        return (me_n, lax.rem(me_t + r, groups))

    def remote(src, dst, send, recv, device):
        return pltpu.make_async_remote_copy(
            src_ref=src,
            dst_ref=dst,
            send_sem=send,
            recv_sem=recv,
            device_id=device,
            device_id_type=MESH,
        )

    def spread(src, dst, send, recv, batch, base=0):
        def one(j, carry):
            peer = plane_peer(BATCHES * j + batch)
            remote(src.at[base + j], dst.at[base + some - batch - j], send, recv, peer).start()
            return carry

        lax.fori_loop(1 - batch, some, one, 0)

    def spread_desc(src, dst, send, recv, low, high):
        at = pl.ds(low, high - low)
        return remote(src.at[at], dst.at[at], send, recv, plane_peer(1))

    def plane_sent(batch):
        return single(PLANE_SENT) if batch == 0 else single(PLANE_SENT_ODD)

    across = min(4, groups // 2)
    deep = groups // (2 * across)
    me_core, me_x, me_z = lax.rem(me_t, 2), lax.rem(me_t // 2, across), me_t // (2 * across)

    def torus_peer(dz, dx, dc):
        z, x, core = lax.rem(me_z + dz, deep), lax.rem(me_x + dx, across), lax.rem(me_core + dc, 2)
        return (me_n, (z * across + x) * 2 + core)

    beside = [torus_peer(0, dx, 0) for dx in range(1, across)]
    greeted = [right, left, torus_peer(0, 0, 1)] + beside
    greeted += [torus_peer(0, dx, 1) for dx in range(1, across)]
    greeted += [torus_peer(dz, 0, dc) for dz in range(1, deep) for dc in range(2)]
    barrier = pltpu.get_barrier_semaphore()
    for device in greeted:
        pl.semaphore_signal(barrier, inc=1, device_id=device, device_id_type=MESH)

    def tok_copy(c):
        return pltpu.make_async_copy(
            tok_hbm.at[:, pl.ds(pl.multiple_of(c * width, width), width)],
            tok.at[c],
            single(TOK_FIRST if c == 0 else TOK_REST),
        )

    def wd_copy(c):
        return pltpu.make_async_copy(
            wd_hbm.at[:, pl.ds(pl.multiple_of(c * width, width), width)], wd.at[c], single(W_DOWN)
        )

    wg_copy = pltpu.make_async_copy(wg_hbm, wg, single(W_GATE))
    wu_copy = pltpu.make_async_copy(wu_hbm, wu, single(W_UP))
    ids_copy = pltpu.make_async_copy(ids_hbm, ids_ref, single(IDS))
    rw_copy = pltpu.make_async_copy(rw_hbm, rw_ref, single(GAINS))
    ids_copy.start()
    rw_copy.start()
    for c in range(chunks):
        tok_copy(c).start()
    wg_copy.start()
    wu_copy.start()
    for c in range(chunks):
        wd_copy(c).start()

    slot = lax.broadcasted_iota(jnp.int32, (slots, rows_tok), 0)
    spot = slot // CAP
    offset = BATCHES * lax.rem(spot, some) + spot // some
    group = lax.rem(me_t + offset, groups)
    ids_copy.wait()
    rw_copy.wait()
    ids = ids_ref[...]
    weights = rw_ref[...].astype(F32)
    member = jnp.zeros((slots, rows_tok), F32)
    weight_a = jnp.zeros((slots, rows_tok), F32)
    weight_b = jnp.zeros((slots, rows_tok), F32)
    for k in range(ids.shape[0]):
        one = jnp.broadcast_to(ids[k : k + 1, :], (slots, rows_tok))
        gain = jnp.broadcast_to(weights[k : k + 1, :], (slots, rows_tok))
        is_a = one == 2 * group
        is_b = one == 2 * group + 1
        weight_a = jnp.where(is_a, gain, weight_a)
        weight_b = jnp.where(is_b, gain, weight_b)
        member = jnp.where(is_a | is_b, jnp.float32(1.0), member)
    before = (
        lax.broadcasted_iota(jnp.int32, (rows_tok, rows_tok), 0)
        < lax.broadcasted_iota(jnp.int32, (rows_tok, rows_tok), 1)
    )
    before = jnp.where(before, jnp.float32(1.0), jnp.float32(0.0)).astype(BF16)
    index = dot(member.astype(BF16), before)
    here = index == lax.rem(slot, CAP).astype(F32)
    place = jnp.where(here, member, jnp.float32(0.0))
    place_ref[...] = place.astype(BF16)
    place_t_ref[...] = jnp.transpose(place).astype(BF16)
    lane = lax.broadcasted_iota(jnp.int32, (rows_tok, LANES), 1)
    low = jnp.where(lane < LANES // 2, jnp.float32(1.0), jnp.float32(0.0))
    spread_w = dot((place * weight_a).astype(BF16), low.astype(BF16)) + dot(
        (place * weight_b).astype(BF16), (1.0 - low).astype(BF16)
    )
    wsb[...] = spread_w.reshape(groups, CAP, LANES).astype(BF16)

    def prepare(c):
        if c == 0:
            tok_copy(0).wait()
        elif c == 1:
            rest = tok.at[pl.ds(1, chunks - 1)]
            pltpu.make_async_copy(rest, rest, single(TOK_REST)).wait()
        parts = []
        for b in range(width // QBLOCK):
            x = tok[c, :, b * QBLOCK : (b + 1) * QBLOCK].astype(F32)
            top = jnp.max(jnp.abs(x), axis=1, keepdims=True)
            scale = ((top + 1e-06) * (1.0 / 448.0)).astype(BF16).astype(F32)
            scale = jnp.broadcast_to(scale, x.shape)
            quantized = (x / scale).astype(BF16)
            parts.append((quantized.astype(F32) * scale).astype(BF16))
        restored = jnp.concatenate(parts, axis=1)
        picked = dot(place_ref[...], restored).reshape(groups, CAP, width).astype(BF16)
        if c == 0:
            zbuf[OWN] = picked
        else:
            for b in range(BATCHES):
                sbuf[b * plain + c - 1] = picked[b * some : (b + 1) * some]

    def send_plane(u):
        if isinstance(u, int):
            spread(sbuf.at[u], rbuf.at[u], plane_sent(u // plain), plane_in(u), u // plain)
            return
        for b in range(BATCHES):

            @pl.when(u // plain == b)
            def _(b=b):
                spread(sbuf.at[u], rbuf.at[u], plane_sent(b), plane_in(u), b)

    def y_send(block, u, sent):
        return (
            remote(block.at[OWN], block.at[LEFT], single(sent), near_sem(u), right),
            remote(block.at[OWN], block.at[RIGHT], single(sent), near_sem(u), left),
        )

    def y_relay(block, u, sent):
        middle = block.shape[1] // 2
        low, high = pl.ds(0, middle), pl.ds(middle, middle)
        return (
            remote(block.at[LEFT, low], block.at[FAR, low], single(sent), far_sem(u), right),
            remote(block.at[RIGHT, high], block.at[FAR, high], single(sent), far_sem(u), left),
        )

    def wait_in(ref, sem):
        remote(ref, ref, single(Y_SENT), sem, right).wait_recv()

    def wait_out(ref, k):
        remote(ref, ref, single(k), near_sem(0), right).wait_send()

    def wait_far(block, u):
        wait_in(block.at[FAR], far_sem(u))

    def flat(ref_value):
        count, cap, lanes = ref_value.shape
        return ref_value.astype(F32).reshape(count * cap, lanes).astype(BF16)

    def arrive(u):
        def gather(low, high):
            wait_in(rbuf.at[u, pl.ds(low, high - low)], plane_in(u))

        def own_too():
            gather(1, some)
            rbuf[u, 0] = sbuf[u, 0]

        if isinstance(u, int):
            own_too()
        else:
            pl.when(u // plain == 0)(own_too)
            pl.when(u // plain == 1)(lambda: gather(0, some))
        xbuf[u, OWN] = flat(rbuf[u])
        for copy in y_send(xbuf.at[u], u, Y_SENT):
            copy.start()

    def pass_on(block, u, sent):
        wait_in(block.at[pl.ds(RIGHT, 2)], near_sem(u))
        for copy in y_relay(block, u, sent):
            copy.start()

    def multiply(u):
        wait_far(xbuf.at[u], u)
        batch = u // plain
        add_chunk(xbuf[u].reshape(nodes * rows, width), batch, u - batch * plain + 1)

    def add_chunk(x, batch, c):
        at = pl.ds(pl.multiple_of(c * width, width), width)
        for e in range(EXP_DEV):
            acc[batch, 2 * e] += dot(x, wg[e, at, :])
            acc[batch, 2 * e + 1] += dot(x, wu[e, at, :])

    def z_piece(batch):
        return zbuf.at[:, pl.ds(batch * some, some)], steps + 1 + batch

    def spread_planes(src, dst, send, recv, batch):
        def one(j, carry):
            peer = plane_peer(BATCHES * j + batch)
            here, there = batch * some + j, batch * some + some - batch - j
            remote(src.at[:, here], dst.at[:, there], send, recv, peer).start()
            return carry

        lax.fori_loop(1 - batch, some, one, 0)

    def wait_planes(ref, sem, batch):
        wait_in(ref.at[:, pl.ds(batch * some + 1 - batch, some - 1 + batch)], sem)

    def z_out(batch):
        wait_far(*z_piece(batch))
        spread_planes(zbuf, zin, single(Z_PLANE_SENT), plane_in(steps + 1 + batch), batch)

    def z_multiply(batch):
        wait_planes(zin, plane_in(steps + 1 + batch), batch)
        if batch == 0:
            zin[:, 0] = zbuf[:, 0]
        x = zin[:, batch * some : (batch + 1) * some].astype(F32)
        add_chunk(x.reshape(nodes * rows, width).astype(BF16), batch, 0)

    def w_project(batch):
        part = dot(hid[batch], wd[plain])
        wbuf[:, batch * some : (batch + 1) * some] = part.reshape(nodes, some, CAP, width).astype(BF16)
        spread_planes(wbuf, win, single(W_PLANE_SENT), back_sem(plain + batch), batch)

    def w_opposite(batch):
        wait_planes(win, back_sem(plain + batch), batch)
        if batch == 0:
            win[:, 0] = wbuf[:, 0]
        mid = some // 2
        for k, device in enumerate((right, left)):
            part = win.at[FAR, pl.ds(batch * some + k * mid, mid)]
            sem = near_sem(steps + 1 + batch)
            remote(part, w_opp_in.at[batch, k], single(W_FAR_SENT), sem, device).start()

    def w_neighbour(batch):
        low, mid, high = batch * some, batch * some + some // 2, (batch + 1) * some
        wait_in(w_opp_in.at[batch], near_sem(steps + 1 + batch))
        w_near[batch, 0, : some // 2] = (
            win[RIGHT, low:mid].astype(F32) + w_opp_in[batch, 0].astype(F32)
        ).astype(BF16)
        w_near[batch, 0, some // 2 :] = win[RIGHT, mid:high]
        w_near[batch, 1, : some // 2] = win[LEFT, low:mid]
        w_near[batch, 1, some // 2 :] = (
            win[LEFT, mid:high].astype(F32) + w_opp_in[batch, 1].astype(F32)
        ).astype(BF16)
        for k, device in enumerate((right, left)):
            sem = far_sem(steps + 1 + batch)
            remote(w_near.at[batch, k], w_near_in.at[batch, k], single(W_NEAR_SENT), sem, device).start()

    def w_finish(batch):
        wait_in(w_near_in.at[batch], far_sem(steps + 1 + batch))
        part = win[OWN, batch * some : (batch + 1) * some].astype(F32)
        part = part + w_near_in[batch, 0].astype(F32) + w_near_in[batch, 1].astype(F32)
        return dot(
            place_t_ref[:, batch * rows : (batch + 1) * rows], part.reshape(rows, width).astype(BF16)
        )

    def activate(batch):
        for e in range(EXP_DEV):
            gate = acc[batch, 2 * e]
            gain = wcol[e, :, batch * rows : (batch + 1) * rows, :].reshape(nodes * rows, LANES)
            gain = jnp.broadcast_to(gain[:, :1], gate.shape)
            value = gate / (1.0 + jnp.exp(-gate)) * acc[batch, 2 * e + 1] * gain
            hid[batch, :, e * ff : (e + 1) * ff] = value.astype(BF16)

    def project(u, first, count):
        batch = u // plain
        return dot(hid[batch, first * rows : (first + count) * rows, :], wd[u - batch * plain])

    def start_opposite(u):
        part = project(u, FAR, 1)
        for k, device in enumerate((right, left)):
            opp[u, k] = part[k * half : (k + 1) * half].astype(BF16)
            remote(opp.at[u, k], opp_in.at[u, k], single(OPP_SENT), near_sem(u), device).start()

    def start_neighbour(u):
        part = project(u, RIGHT, 2)
        wait_in(opp_in.at[u], near_sem(u))
        near[u, 0, :half] = (part[:half] + opp_in[u, 0].astype(F32)).astype(BF16)
        near[u, 0, half:] = part[half:rows].astype(BF16)
        near[u, 1, :half] = part[rows : rows + half].astype(BF16)
        near[u, 1, half:] = (part[rows + half :] + opp_in[u, 1].astype(F32)).astype(BF16)
        for k, device in enumerate((right, left)):
            remote(near.at[u, k], near_in.at[u, k], single(NEAR_SENT), far_sem(u), device).start()

    def finish(u):
        part = project(u, OWN, 1)
        wait_in(near_in.at[u], far_sem(u))
        part = part + near_in[u, 0].astype(F32) + near_in[u, 1].astype(F32)
        batch = u // plain
        c, base = u - batch * plain, batch * some
        rsb[c, pl.ds(base, some)] = part.reshape(some, CAP, width).astype(BF16)
        spread(rsb.at[c], rrb.at[c], single(BACK_SENT), back_sem(c), batch, base)

    def collect(c):
        wait_in(rrb.at[c, pl.ds(1, groups - 1)], back_sem(c))
        rrb[c, 0] = rsb[c, 0]
        total = jnp.zeros((rows_tok, width), F32)
        for b in range(BATCHES):
            back = flat(rrb[c, b * some : (b + 1) * some])
            total += dot(place_t_ref[:, b * rows : (b + 1) * rows], back)
        out_ref[:, pl.ds(pl.multiple_of(c * width, width), width)] = total.astype(BF16)

    prepare(0)
    pl.semaphore_wait(barrier, len(greeted))
    for b in range(BATCHES):
        for copy in y_send(*z_piece(b), Z_Y_SENT):
            copy.start()
    acc[...] = jnp.zeros_like(acc)
    for device in beside:
        pl.semaphore_signal(round_sem, inc=1, device_id=device, device_id_type=MESH)
    prepare(1)
    pl.semaphore_wait(round_sem, len(beside))
    for c in range(2, chunks):
        if c - 2 < EARLY:
            send_plane(c - 2)
        prepare(c)
        if c == 4:
            pass_on(*z_piece(0), Z_RELAY_SENT)
    for b in range(BATCHES):
        at = pl.ds(b * some, some)
        spread(wsb.at[at], wrb.at[at], single(GAIN_PLANE_SENT), plane_in(steps), b)
    arrive(0)
    pass_on(*z_piece(1), Z_RELAY_SENT)

    lag_y, lag_x, lag_m = 0, 2, 4
    lag_o = steps + 1
    lag_n, lag_f, lag_c = lag_o + 2, lag_o + 4, lag_o + 6

    def stage(s, lag, first, last, work):
        @pl.when((s >= lag + first) & (s < lag + last))
        def _():
            work(s - lag)

    def at_step(s, step, work, *args):
        @pl.when(s == step)
        def _():
            work(*args)

    def share_weights():
        wait_in(wrb.at[pl.ds(1, groups - 1)], plane_in(steps))
        wrb[0] = wsb[0]
        turned = jnp.transpose(wrb[...].astype(F32).reshape(slots, LANES)).astype(BF16)
        for e in range(EXP_DEV):
            first = e * (LANES // EXP_DEV)
            wx[OWN, e * PACK : (e + 1) * PACK] = turned[first : first + PACK]
        for copy in y_send(wx, steps, GAIN_Y_SENT):
            copy.start()

    def have_gate_up():
        wg_copy.wait()
        wu_copy.wait()
        pltpu.make_async_copy(wd, wd, single(W_DOWN)).wait()

    def have_weights():
        wait_far(wx, steps)
        for e in range(EXP_DEV):
            for plane in range(nodes):
                line = wx[plane, e * PACK : e * PACK + 1, :].astype(F32)
                wcol[e, plane] = jnp.transpose(jnp.broadcast_to(line, (LANES, slots)))

    def turn(batch):
        z_multiply(batch)
        activate(batch)
        w_project(batch)

    def w_last():
        total = w_finish(0) + w_finish(1)
        out_ref[:, plain * width :] = total.astype(BF16)

    def send_two(k):
        send_plane(EARLY + 2 * k)
        send_plane(EARLY + 1 + 2 * k)

    def whole(s, carry):
        stage(s, 0, 0, (steps - EARLY) // 2, send_two)
        stage(s, lag_y, 1, steps, arrive)
        at_step(s, 3, share_weights)
        at_step(s, 3, have_gate_up)
        stage(s, lag_x, 0, steps, lambda u: pass_on(xbuf.at[u], u, RELAY_SENT))
        at_step(s, 5, pass_on, wx, steps, GAIN_RELAY_SENT)
        at_step(s, 4, z_out, 0)
        at_step(s, 5, z_out, 1)
        stage(s, lag_m, 0, steps, multiply)
        at_step(s, 8, have_weights)
        at_step(s, steps, turn, 0)
        at_step(s, lag_m + steps - 1, turn, 1)
        stage(s, lag_o, 0, steps, start_opposite)
        at_step(s, lag_o + steps, w_opposite, 0)
        at_step(s, lag_o + steps + 1, w_opposite, 1)
        stage(s, lag_n, 0, steps, start_neighbour)
        at_step(s, lag_n + steps, w_neighbour, 0)
        at_step(s, lag_n + steps + 1, w_neighbour, 1)
        stage(s, lag_f, 0, steps, finish)
        stage(s, lag_c + steps - plain, 0, plain, collect)
        at_step(s, lag_f + steps + 1, w_last)
        return carry

    lax.fori_loop(0, lag_f + steps + 2, whole, 0)

    first, second = pl.ds(0, plain), pl.ds(plain, plain)
    wait_out(sbuf.at[first, pl.ds(1, some - 1)], PLANE_SENT)
    wait_out(sbuf.at[second], PLANE_SENT_ODD)
    wait_out(wsb.at[pl.ds(1, groups - 1)], GAIN_PLANE_SENT)
    wait_out(zbuf.at[:, pl.ds(1, groups - 1)], Z_PLANE_SENT)
    wait_out(wbuf.at[:, pl.ds(1, groups - 1)], W_PLANE_SENT)
    wait_out(rsb.at[:, pl.ds(1, groups - 1)], BACK_SENT)
    wait_out(xbuf.at[:, pl.ds(RIGHT, 2)], Y_SENT)
    wait_out(xbuf.at[:, FAR], RELAY_SENT)
    wait_out(wx.at[pl.ds(RIGHT, 2)], GAIN_Y_SENT)
    wait_out(wx.at[FAR], GAIN_RELAY_SENT)
    wait_out(zbuf.at[pl.ds(RIGHT, 2)], Z_Y_SENT)
    wait_out(zbuf.at[FAR], Z_RELAY_SENT)
    wait_out(opp, OPP_SENT)
    wait_out(near, NEAR_SENT)
    wait_out(w_opp_in, W_FAR_SENT)
    wait_out(w_near, W_NEAR_SENT)


def solution(mesh):
    nodes, groups = mesh.shape["node"], mesh.shape["torus"]

    def shards(tokens, expert_ids, route_weight, w_gate, w_up, w_down):
        rows_tok, depth = tokens.shape
        ff = w_gate.shape[2]
        width = min(CHUNK, depth)
        chunks = depth // width
        slots = groups * CAP
        steps = BATCHES * (chunks - 1)
        some = groups // BATCHES
        rows = some * CAP
        anywhere = pl.BlockSpec(memory_space=pl.ANY)
        inside = pl.BlockSpec(memory_space=pltpu.VMEM)
        block = pltpu.VMEM((steps, some, CAP, width), BF16)
        planes = pltpu.VMEM((nodes, groups, CAP, width), BF16)
        piece = pltpu.VMEM((BATCHES, 2, some, CAP, width), BF16)
        returned = pltpu.VMEM((chunks - 1, groups, CAP, width), BF16)
        arrivals = 3 * (steps + 1 + BATCHES) + chunks - 1 + BATCHES
        return pl.pallas_call(
            functools.partial(layer, nodes, groups),
            out_shape=pltpu.VMEM((rows_tok, depth), BF16),
            in_specs=[anywhere] * 6,
            out_specs=inside,
            scratch_shapes=[
                pltpu.VMEM(expert_ids.shape[::-1], jnp.int32),
                pltpu.VMEM(route_weight.shape[::-1], BF16),
                pltpu.VMEM((chunks, rows_tok, width), BF16),
                pltpu.VMEM(w_gate.shape, BF16),
                pltpu.VMEM(w_up.shape, BF16),
                pltpu.VMEM((chunks, EXP_DEV * ff, width), BF16),
                block,
                block,
                pltpu.VMEM((steps, nodes, rows, width), BF16),
                pltpu.VMEM((groups, CAP, LANES), BF16),
                pltpu.VMEM((groups, CAP, LANES), BF16),
                pltpu.VMEM((nodes, EXP_DEV * PACK, slots), BF16),
                pltpu.VMEM((EXP_DEV, nodes, slots, LANES), F32),
                pltpu.VMEM((BATCHES, 2 * EXP_DEV, nodes * rows, ff), F32),
                pltpu.VMEM((BATCHES, nodes * rows, EXP_DEV * ff), BF16),
                pltpu.VMEM((steps, 2, rows // 2, width), BF16),
                pltpu.VMEM((steps, 2, rows // 2, width), BF16),
                pltpu.VMEM((steps, 2, rows, width), BF16),
                pltpu.VMEM((steps, 2, rows, width), BF16),
                returned,
                returned,
                planes,
                planes,
                planes,
                planes,
                pltpu.VMEM((BATCHES, 2, some // 2, CAP, width), BF16),
                piece,
                piece,
                pltpu.VMEM((slots, rows_tok), BF16),
                pltpu.VMEM((rows_tok, slots), BF16),
                pltpu.SemaphoreType.DMA((arrivals + SINGLES,)),
                pltpu.SemaphoreType.REGULAR,
            ],
            compiler_params=pltpu.CompilerParams(
                collective_id=0, has_side_effects=True, vmem_limit_bytes=59000000
            ),
        )(
            tokens,
            expert_ids.T,
            route_weight.T,
            w_gate,
            w_up,
            w_down.reshape(EXP_DEV * ff, depth),
        )

    placed = (
        P(("node", "torus"), None),
        P(("node", "torus"), None),
        P(("node", "torus"), None),
        P("torus", None, "node"),
        P("torus", None, "node"),
        P("torus", "node", None),
    )
    return jax.shard_map(
        shards, mesh=mesh, in_specs=placed, out_specs=P(("node", "torus"), None), check_vma=False
    )
```

```python
import functools

import jax
import jax.numpy as jnp
from jax import lax
from jax.experimental import pallas as pl
from jax.experimental.pallas import tpu as pltpu
from jax.sharding import PartitionSpec as P

EXP_DEV = 2
CAP = 4
QBLOCK = 128
LANES = 128
CHUNK = 1024
BATCHES = 2
EARLY = 4
PACK = 16
MESH = pl.DeviceIdType.MESH
F32 = jnp.float32
BF16 = jnp.bfloat16

(
    TOK_FIRST,
    TOK_REST,
    W_GATE,
    W_UP,
    W_DOWN,
    IDS,
    GAINS,
    PLANE_SENT,
    GAIN_PLANE_SENT,
    Z_PLANE_SENT,
    Y_SENT,
    RELAY_SENT,
    GAIN_Y_SENT,
    GAIN_RELAY_SENT,
    Z_Y_SENT,
    Z_RELAY_SENT,
    OPP_SENT,
    NEAR_SENT,
    BACK_SENT,
    W_FAR_SENT,
    W_NEAR_SENT,
    W_PLANE_SENT,
    PLANE_SENT_ODD,
    SINGLES,
) = range(24)


def dot(a, b):
    return jnp.dot(a, b, preferred_element_type=F32)


def layer(
    nodes,
    groups,
    tok_hbm,
    ids_hbm,
    rw_hbm,
    wg_hbm,
    wu_hbm,
    wd_hbm,
    out_ref,
    ids_ref,
    rw_ref,
    tok,
    wg,
    wu,
    wd,
    sbuf,
    rbuf,
    xbuf,
    wsb,
    wrb,
    wx,
    wcol,
    acc,
    hid,
    opp,
    opp_in,
    near,
    near_in,
    rsb,
    rrb,
    zbuf,
    zin,
    wbuf,
    win,
    w_opp_in,
    w_near,
    w_near_in,
    place_ref,
    place_t_ref,
    sems,
    round_sem,
):
    chunks, rows_tok, width = tok.shape
    plain = chunks - 1
    steps = BATCHES * plain
    some = groups // BATCHES
    slots = groups * CAP
    rows = some * CAP
    half = rows // 2
    ff = wg.shape[2]
    me_n = lax.axis_index("node")
    me_t = lax.axis_index("torus")
    right = (lax.rem(me_n + 1, nodes), me_t)
    left = (lax.rem(me_n + nodes - 1, nodes), me_t)
    OWN, RIGHT, LEFT, FAR = range(4)

    table = steps + 1 + BATCHES

    def plane_in(u):
        return sems.at[u]

    def near_sem(u):
        return sems.at[table + u]

    def far_sem(u):
        return sems.at[2 * table + u]

    def back_sem(c):
        return sems.at[3 * table + c]

    def single(k):
        return sems.at[3 * table + plain + BATCHES + k]

    def plane_peer(r):
        return (me_n, lax.rem(me_t + r, groups))

    def remote(src, dst, send, recv, device):
        return pltpu.make_async_remote_copy(
            src_ref=src,
            dst_ref=dst,
            send_sem=send,
            recv_sem=recv,
            device_id=device,
            device_id_type=MESH,
        )

    def spread(src, dst, send, recv, batch, base=0):
        def one(j, carry):
            peer = plane_peer(BATCHES * j + batch)
            remote(src.at[base + j], dst.at[base + some - batch - j], send, recv, peer).start()
            return carry

        lax.fori_loop(1 - batch, some, one, 0)

    def spread_desc(src, dst, send, recv, low, high):
        at = pl.ds(low, high - low)
        return remote(src.at[at], dst.at[at], send, recv, plane_peer(1))

    def plane_sent(batch):
        return single(PLANE_SENT) if batch == 0 else single(PLANE_SENT_ODD)

    across = min(4, groups // 2)
    deep = groups // (2 * across)
    me_core, me_x, me_z = lax.rem(me_t, 2), lax.rem(me_t // 2, across), me_t // (2 * across)

    def torus_peer(dz, dx, dc):
        z, x, core = lax.rem(me_z + dz, deep), lax.rem(me_x + dx, across), lax.rem(me_core + dc, 2)
        return (me_n, (z * across + x) * 2 + core)

    beside = [torus_peer(0, dx, 0) for dx in range(1, across)]
    greeted = [right, left, torus_peer(0, 0, 1)] + beside
    greeted += [torus_peer(0, dx, 1) for dx in range(1, across)]
    greeted += [torus_peer(dz, 0, dc) for dz in range(1, deep) for dc in range(2)]
    barrier = pltpu.get_barrier_semaphore()
    for device in greeted:
        pl.semaphore_signal(barrier, inc=1, device_id=device, device_id_type=MESH)

    def tok_copy(c):
        return pltpu.make_async_copy(
            tok_hbm.at[:, pl.ds(pl.multiple_of(c * width, width), width)],
            tok.at[c],
            single(TOK_FIRST if c == 0 else TOK_REST),
        )

    def wd_copy(c):
        return pltpu.make_async_copy(
            wd_hbm.at[:, pl.ds(pl.multiple_of(c * width, width), width)], wd.at[c], single(W_DOWN)
        )

    wg_copy = pltpu.make_async_copy(wg_hbm, wg, single(W_GATE))
    wu_copy = pltpu.make_async_copy(wu_hbm, wu, single(W_UP))
    ids_copy = pltpu.make_async_copy(ids_hbm, ids_ref, single(IDS))
    rw_copy = pltpu.make_async_copy(rw_hbm, rw_ref, single(GAINS))
    ids_copy.start()
    rw_copy.start()
    for c in range(chunks):
        tok_copy(c).start()
    wg_copy.start()
    wu_copy.start()
    for c in range(chunks):
        wd_copy(c).start()

    slot = lax.broadcasted_iota(jnp.int32, (slots, rows_tok), 0)
    spot = slot // CAP
    offset = BATCHES * lax.rem(spot, some) + spot // some
    group = lax.rem(me_t + offset, groups)
    ids_copy.wait()
    rw_copy.wait()
    ids = ids_ref[...]
    weights = rw_ref[...].astype(F32)
    member = jnp.zeros((slots, rows_tok), F32)
    weight_a = jnp.zeros((slots, rows_tok), F32)
    weight_b = jnp.zeros((slots, rows_tok), F32)
    for k in range(ids.shape[0]):
        one = jnp.broadcast_to(ids[k : k + 1, :], (slots, rows_tok))
        gain = jnp.broadcast_to(weights[k : k + 1, :], (slots, rows_tok))
        is_a = one == 2 * group
        is_b = one == 2 * group + 1
        weight_a = jnp.where(is_a, gain, weight_a)
        weight_b = jnp.where(is_b, gain, weight_b)
        member = jnp.where(is_a | is_b, jnp.float32(1.0), member)
    before = (
        lax.broadcasted_iota(jnp.int32, (rows_tok, rows_tok), 0)
        < lax.broadcasted_iota(jnp.int32, (rows_tok, rows_tok), 1)
    )
    before = jnp.where(before, jnp.float32(1.0), jnp.float32(0.0)).astype(BF16)
    index = dot(member.astype(BF16), before)
    here = index == lax.rem(slot, CAP).astype(F32)
    place = jnp.where(here, member, jnp.float32(0.0))
    place_ref[...] = place.astype(BF16)
    place_t_ref[...] = jnp.transpose(place).astype(BF16)
    lane = lax.broadcasted_iota(jnp.int32, (rows_tok, LANES), 1)
    low = jnp.where(lane < LANES // 2, jnp.float32(1.0), jnp.float32(0.0))
    spread_w = dot((place * weight_a).astype(BF16), low.astype(BF16)) + dot(
        (place * weight_b).astype(BF16), (1.0 - low).astype(BF16)
    )
    wsb[...] = spread_w.reshape(groups, CAP, LANES).astype(BF16)

    def prepare(c):
        if c == 0:
            tok_copy(0).wait()
        elif c == 1:
            rest = tok.at[pl.ds(1, chunks - 1)]
            pltpu.make_async_copy(rest, rest, single(TOK_REST)).wait()
        parts = []
        for b in range(width // QBLOCK):
            x = tok[c, :, b * QBLOCK : (b + 1) * QBLOCK].astype(F32)
            top = jnp.max(jnp.abs(x), axis=1, keepdims=True)
            scale = ((top + 1e-06) * (1.0 / 448.0)).astype(BF16).astype(F32)
            scale = jnp.broadcast_to(scale, x.shape)
            quantized = (x / scale).astype(BF16)
            parts.append((quantized.astype(F32) * scale).astype(BF16))
        restored = jnp.concatenate(parts, axis=1)
        picked = dot(place_ref[...], restored).reshape(groups, CAP, width).astype(BF16)
        if c == 0:
            zbuf[OWN] = picked
        else:
            for b in range(BATCHES):
                sbuf[b * plain + c - 1] = picked[b * some : (b + 1) * some]

    def send_plane(u):
        if isinstance(u, int):
            spread(sbuf.at[u], rbuf.at[u], plane_sent(u // plain), plane_in(u), u // plain)
            return
        for b in range(BATCHES):

            @pl.when(u // plain == b)
            def _(b=b):
                spread(sbuf.at[u], rbuf.at[u], plane_sent(b), plane_in(u), b)

    def y_send(block, u, sent):
        return (
            remote(block.at[OWN], block.at[LEFT], single(sent), near_sem(u), right),
            remote(block.at[OWN], block.at[RIGHT], single(sent), near_sem(u), left),
        )

    def y_relay(block, u, sent):
        middle = block.shape[1] // 2
        low, high = pl.ds(0, middle), pl.ds(middle, middle)
        return (
            remote(block.at[LEFT, low], block.at[FAR, low], single(sent), far_sem(u), right),
            remote(block.at[RIGHT, high], block.at[FAR, high], single(sent), far_sem(u), left),
        )

    def wait_in(ref, sem):
        remote(ref, ref, single(Y_SENT), sem, right).wait_recv()

    def wait_out(ref, k):
        remote(ref, ref, single(k), near_sem(0), right).wait_send()

    def wait_far(block, u):
        wait_in(block.at[FAR], far_sem(u))

    def flat(ref_value):
        count, cap, lanes = ref_value.shape
        return ref_value.astype(F32).reshape(count * cap, lanes).astype(BF16)

    def arrive(u):
        def gather(low, high):
            wait_in(rbuf.at[u, pl.ds(low, high - low)], plane_in(u))

        def own_too():
            gather(1, some)
            rbuf[u, 0] = sbuf[u, 0]

        if isinstance(u, int):
            own_too()
        else:
            pl.when(u // plain == 0)(own_too)
            pl.when(u // plain == 1)(lambda: gather(0, some))
        xbuf[u, OWN] = flat(rbuf[u])
        for copy in y_send(xbuf.at[u], u, Y_SENT):
            copy.start()

    def pass_on(block, u, sent):
        wait_in(block.at[pl.ds(RIGHT, 2)], near_sem(u))
        for copy in y_relay(block, u, sent):
            copy.start()

    def multiply(u):
        wait_far(xbuf.at[u], u)
        batch = u // plain
        add_chunk(xbuf[u].reshape(nodes * rows, width), batch, u - batch * plain + 1)

    def add_chunk(x, batch, c):
        at = pl.ds(pl.multiple_of(c * width, width), width)
        for e in range(EXP_DEV):
            acc[batch, 2 * e] += dot(x, wg[e, at, :])
            acc[batch, 2 * e + 1] += dot(x, wu[e, at, :])

    def z_piece(batch):
        return zbuf.at[:, pl.ds(batch * some, some)], steps + 1 + batch

    def spread_planes(src, dst, send, recv, batch):
        def one(j, carry):
            peer = plane_peer(BATCHES * j + batch)
            here, there = batch * some + j, batch * some + some - batch - j
            remote(src.at[:, here], dst.at[:, there], send, recv, peer).start()
            return carry

        lax.fori_loop(1 - batch, some, one, 0)

    def wait_planes(ref, sem, batch):
        wait_in(ref.at[:, pl.ds(batch * some + 1 - batch, some - 1 + batch)], sem)

    def z_out(batch):
        wait_far(*z_piece(batch))
        spread_planes(zbuf, zin, single(Z_PLANE_SENT), plane_in(steps + 1 + batch), batch)

    def z_multiply(batch):
        wait_planes(zin, plane_in(steps + 1 + batch), batch)
        if batch == 0:
            zin[:, 0] = zbuf[:, 0]
        x = zin[:, batch * some : (batch + 1) * some].astype(F32)
        add_chunk(x.reshape(nodes * rows, width).astype(BF16), batch, 0)

    def w_project(batch):
        part = dot(hid[batch], wd[plain])
        wbuf[:, batch * some : (batch + 1) * some] = part.reshape(nodes, some, CAP, width).astype(BF16)
        spread_planes(wbuf, win, single(W_PLANE_SENT), back_sem(plain + batch), batch)

    def w_opposite(batch):
        wait_planes(win, back_sem(plain + batch), batch)
        if batch == 0:
            win[:, 0] = wbuf[:, 0]
        mid = some // 2
        for k, device in enumerate((right, left)):
            part = win.at[FAR, pl.ds(batch * some + k * mid, mid)]
            sem = near_sem(steps + 1 + batch)
            remote(part, w_opp_in.at[batch, k], single(W_FAR_SENT), sem, device).start()

    def w_neighbour(batch):
        low, mid, high = batch * some, batch * some + some // 2, (batch + 1) * some
        wait_in(w_opp_in.at[batch], near_sem(steps + 1 + batch))
        w_near[batch, 0, : some // 2] = (
            win[RIGHT, low:mid].astype(F32) + w_opp_in[batch, 0].astype(F32)
        ).astype(BF16)
        w_near[batch, 0, some // 2 :] = win[RIGHT, mid:high]
        w_near[batch, 1, : some // 2] = win[LEFT, low:mid]
        w_near[batch, 1, some // 2 :] = (
            win[LEFT, mid:high].astype(F32) + w_opp_in[batch, 1].astype(F32)
        ).astype(BF16)
        for k, device in enumerate((right, left)):
            sem = far_sem(steps + 1 + batch)
            remote(w_near.at[batch, k], w_near_in.at[batch, k], single(W_NEAR_SENT), sem, device).start()

    def w_finish(batch):
        wait_in(w_near_in.at[batch], far_sem(steps + 1 + batch))
        part = win[OWN, batch * some : (batch + 1) * some].astype(F32)
        part = part + w_near_in[batch, 0].astype(F32) + w_near_in[batch, 1].astype(F32)
        return dot(
            place_t_ref[:, batch * rows : (batch + 1) * rows], part.reshape(rows, width).astype(BF16)
        )

    def activate(batch):
        for e in range(EXP_DEV):
            gate = acc[batch, 2 * e]
            gain = wcol[e, :, batch * rows : (batch + 1) * rows, :].reshape(nodes * rows, LANES)
            gain = jnp.broadcast_to(gain[:, :1], gate.shape)
            value = gate / (1.0 + jnp.exp(-gate)) * acc[batch, 2 * e + 1] * gain
            hid[batch, :, e * ff : (e + 1) * ff] = value.astype(BF16)

    def project(u, first, count):
        batch = u // plain
        return dot(hid[batch, first * rows : (first + count) * rows, :], wd[u - batch * plain])

    def start_opposite(u):
        part = project(u, FAR, 1)
        for k, device in enumerate((right, left)):
            opp[u, k] = part[k * half : (k + 1) * half].astype(BF16)
            remote(opp.at[u, k], opp_in.at[u, k], single(OPP_SENT), near_sem(u), device).start()

    def start_neighbour(u):
        part = project(u, RIGHT, 2)
        wait_in(opp_in.at[u], near_sem(u))
        near[u, 0, :half] = (part[:half] + opp_in[u, 0].astype(F32)).astype(BF16)
        near[u, 0, half:] = part[half:rows].astype(BF16)
        near[u, 1, :half] = part[rows : rows + half].astype(BF16)
        near[u, 1, half:] = (part[rows + half :] + opp_in[u, 1].astype(F32)).astype(BF16)
        for k, device in enumerate((right, left)):
            remote(near.at[u, k], near_in.at[u, k], single(NEAR_SENT), far_sem(u), device).start()

    def finish(u):
        part = project(u, OWN, 1)
        wait_in(near_in.at[u], far_sem(u))
        part = part + near_in[u, 0].astype(F32) + near_in[u, 1].astype(F32)
        batch = u // plain
        c, base = u - batch * plain, batch * some
        rsb[c, pl.ds(base, some)] = part.reshape(some, CAP, width).astype(BF16)
        spread(rsb.at[c], rrb.at[c], single(BACK_SENT), back_sem(c), batch, base)

    def collect(c):
        wait_in(rrb.at[c, pl.ds(1, groups - 1)], back_sem(c))
        rrb[c, 0] = rsb[c, 0]
        total = jnp.zeros((rows_tok, width), F32)
        for b in range(BATCHES):
            back = flat(rrb[c, b * some : (b + 1) * some])
            total += dot(place_t_ref[:, b * rows : (b + 1) * rows], back)
        out_ref[:, pl.ds(pl.multiple_of(c * width, width), width)] = total.astype(BF16)

    prepare(0)
    pl.semaphore_wait(barrier, len(greeted))
    for b in range(BATCHES):
        for copy in y_send(*z_piece(b), Z_Y_SENT):
            copy.start()
    acc[...] = jnp.zeros_like(acc)
    for device in beside:
        pl.semaphore_signal(round_sem, inc=1, device_id=device, device_id_type=MESH)
    prepare(1)
    pl.semaphore_wait(round_sem, len(beside))
    for c in range(2, chunks):
        if c - 2 < EARLY:
            send_plane(c - 2)
        prepare(c)
        if c == 4:
            pass_on(*z_piece(0), Z_RELAY_SENT)
    for b in range(BATCHES):
        at = pl.ds(b * some, some)
        spread(wsb.at[at], wrb.at[at], single(GAIN_PLANE_SENT), plane_in(steps), b)
    arrive(0)
    pass_on(*z_piece(1), Z_RELAY_SENT)

    lag_y, lag_x, lag_m = 0, 2, 4
    lag_o = steps
    lag_n, lag_f, lag_c = lag_o + 2, lag_o + 4, lag_o + 6

    def stage(s, lag, first, last, work):
        @pl.when((s >= lag + first) & (s < lag + last))
        def _():
            work(s - lag)

    def at_step(s, step, work, *args):
        @pl.when(s == step)
        def _():
            work(*args)

    def share_weights():
        wait_in(wrb.at[pl.ds(1, groups - 1)], plane_in(steps))
        wrb[0] = wsb[0]
        turned = jnp.transpose(wrb[...].astype(F32).reshape(slots, LANES)).astype(BF16)
        for e in range(EXP_DEV):
            first = e * (LANES // EXP_DEV)
            wx[OWN, e * PACK : (e + 1) * PACK] = turned[first : first + PACK]
        for copy in y_send(wx, steps, GAIN_Y_SENT):
            copy.start()

    def have_gate_up():
        wg_copy.wait()
        wu_copy.wait()
        pltpu.make_async_copy(wd, wd, single(W_DOWN)).wait()

    def have_weights():
        wait_far(wx, steps)
        for e in range(EXP_DEV):
            for plane in range(nodes):
                line = wx[plane, e * PACK : e * PACK + 1, :].astype(F32)
                wcol[e, plane] = jnp.transpose(jnp.broadcast_to(line, (LANES, slots)))

    def turn(batch):
        z_multiply(batch)
        activate(batch)
        w_project(batch)

    def w_last():
        total = w_finish(0) + w_finish(1)
        out_ref[:, plain * width :] = total.astype(BF16)

    def send_two(k):
        send_plane(EARLY + 2 * k)
        send_plane(EARLY + 1 + 2 * k)

    def whole(s, carry):
        stage(s, 0, 0, (steps - EARLY) // 2, send_two)
        stage(s, lag_y, 1, steps, arrive)
        at_step(s, 3, share_weights)
        at_step(s, 3, have_gate_up)
        stage(s, lag_x, 0, steps, lambda u: pass_on(xbuf.at[u], u, RELAY_SENT))
        at_step(s, 5, pass_on, wx, steps, GAIN_RELAY_SENT)
        at_step(s, 4, z_out, 0)
        at_step(s, 5, z_out, 1)
        stage(s, lag_m, 0, steps, multiply)
        at_step(s, 8, have_weights)
        at_step(s, steps, turn, 0)
        at_step(s, lag_m + steps - 1, turn, 1)
        stage(s, lag_o, 0, steps, start_opposite)
        at_step(s, lag_o + steps, w_opposite, 0)
        stage(s, lag_n, 0, steps, start_neighbour)
        at_step(s, lag_o + steps + 1, w_opposite, 1)
        at_step(s, lag_n + steps, w_neighbour, 0)
        stage(s, lag_f, 0, steps, finish)
        at_step(s, lag_n + steps + 1, w_neighbour, 1)
        stage(s, lag_c + steps - plain, 0, plain, collect)
        at_step(s, lag_f + steps + 1, w_last)
        return carry

    lax.fori_loop(0, lag_f + steps + 2, whole, 0)

    first, second = pl.ds(0, plain), pl.ds(plain, plain)
    wait_out(sbuf.at[first, pl.ds(1, some - 1)], PLANE_SENT)
    wait_out(sbuf.at[second], PLANE_SENT_ODD)
    wait_out(wsb.at[pl.ds(1, groups - 1)], GAIN_PLANE_SENT)
    wait_out(zbuf.at[:, pl.ds(1, groups - 1)], Z_PLANE_SENT)
    wait_out(wbuf.at[:, pl.ds(1, groups - 1)], W_PLANE_SENT)
    wait_out(rsb.at[:, pl.ds(1, groups - 1)], BACK_SENT)
    wait_out(xbuf.at[:, pl.ds(RIGHT, 2)], Y_SENT)
    wait_out(xbuf.at[:, FAR], RELAY_SENT)
    wait_out(wx.at[pl.ds(RIGHT, 2)], GAIN_Y_SENT)
    wait_out(wx.at[FAR], GAIN_RELAY_SENT)
    wait_out(zbuf.at[pl.ds(RIGHT, 2)], Z_Y_SENT)
    wait_out(zbuf.at[FAR], Z_RELAY_SENT)
    wait_out(opp, OPP_SENT)
    wait_out(near, NEAR_SENT)
    wait_out(w_opp_in, W_FAR_SENT)
    wait_out(w_near, W_NEAR_SENT)


def solution(mesh):
    nodes, groups = mesh.shape["node"], mesh.shape["torus"]

    def shards(tokens, expert_ids, route_weight, w_gate, w_up, w_down):
        rows_tok, depth = tokens.shape
        ff = w_gate.shape[2]
        width = min(CHUNK, depth)
        chunks = depth // width
        slots = groups * CAP
        steps = BATCHES * (chunks - 1)
        some = groups // BATCHES
        rows = some * CAP
        anywhere = pl.BlockSpec(memory_space=pl.ANY)
        inside = pl.BlockSpec(memory_space=pltpu.VMEM)
        block = pltpu.VMEM((steps, some, CAP, width), BF16)
        planes = pltpu.VMEM((nodes, groups, CAP, width), BF16)
        piece = pltpu.VMEM((BATCHES, 2, some, CAP, width), BF16)
        returned = pltpu.VMEM((chunks - 1, groups, CAP, width), BF16)
        arrivals = 3 * (steps + 1 + BATCHES) + chunks - 1 + BATCHES
        return pl.pallas_call(
            functools.partial(layer, nodes, groups),
            out_shape=pltpu.VMEM((rows_tok, depth), BF16),
            in_specs=[anywhere] * 6,
            out_specs=inside,
            scratch_shapes=[
                pltpu.VMEM(expert_ids.shape[::-1], jnp.int32),
                pltpu.VMEM(route_weight.shape[::-1], BF16),
                pltpu.VMEM((chunks, rows_tok, width), BF16),
                pltpu.VMEM(w_gate.shape, BF16),
                pltpu.VMEM(w_up.shape, BF16),
                pltpu.VMEM((chunks, EXP_DEV * ff, width), BF16),
                block,
                block,
                pltpu.VMEM((steps, nodes, rows, width), BF16),
                pltpu.VMEM((groups, CAP, LANES), BF16),
                pltpu.VMEM((groups, CAP, LANES), BF16),
                pltpu.VMEM((nodes, EXP_DEV * PACK, slots), BF16),
                pltpu.VMEM((EXP_DEV, nodes, slots, LANES), F32),
                pltpu.VMEM((BATCHES, 2 * EXP_DEV, nodes * rows, ff), F32),
                pltpu.VMEM((BATCHES, nodes * rows, EXP_DEV * ff), BF16),
                pltpu.VMEM((steps, 2, rows // 2, width), BF16),
                pltpu.VMEM((steps, 2, rows // 2, width), BF16),
                pltpu.VMEM((steps, 2, rows, width), BF16),
                pltpu.VMEM((steps, 2, rows, width), BF16),
                returned,
                returned,
                planes,
                planes,
                planes,
                planes,
                pltpu.VMEM((BATCHES, 2, some // 2, CAP, width), BF16),
                piece,
                piece,
                pltpu.VMEM((slots, rows_tok), BF16),
                pltpu.VMEM((rows_tok, slots), BF16),
                pltpu.SemaphoreType.DMA((arrivals + SINGLES,)),
                pltpu.SemaphoreType.REGULAR,
            ],
            compiler_params=pltpu.CompilerParams(
                collective_id=0, has_side_effects=True, vmem_limit_bytes=59000000
            ),
        )(
            tokens,
            expert_ids.T,
            route_weight.T,
            w_gate,
            w_up,
            w_down.reshape(EXP_DEV * ff, depth),
        )

    placed = (
        P(("node", "torus"), None),
        P(("node", "torus"), None),
        P(("node", "torus"), None),
        P("torus", None, "node"),
        P("torus", None, "node"),
        P("torus", "node", None),
    )
    return jax.shard_map(
        shards, mesh=mesh, in_specs=placed, out_specs=P(("node", "torus"), None), check_vma=False
    )
```

```python
import functools

import jax
import jax.numpy as jnp
from jax import lax
from jax.experimental import pallas as pl
from jax.experimental.pallas import tpu as pltpu
from jax.sharding import PartitionSpec as P

EXP_DEV = 2
CAP = 4
QBLOCK = 128
LANES = 128
CHUNK = 1024
BATCHES = 2
EARLY = 2
PACK = 16
MESH = pl.DeviceIdType.MESH
F32 = jnp.float32
BF16 = jnp.bfloat16

(
    TOK_FIRST,
    TOK_REST,
    W_GATE,
    W_UP,
    W_DOWN,
    IDS,
    GAINS,
    PLANE_SENT,
    GAIN_PLANE_SENT,
    Z_PLANE_SENT,
    Y_SENT,
    RELAY_SENT,
    GAIN_Y_SENT,
    GAIN_RELAY_SENT,
    Z_Y_SENT,
    Z_RELAY_SENT,
    OPP_SENT,
    NEAR_SENT,
    BACK_SENT,
    W_FAR_SENT,
    W_NEAR_SENT,
    W_PLANE_SENT,
    PLANE_SENT_ODD,
    SINGLES,
) = range(24)


def dot(a, b):
    return jnp.dot(a, b, preferred_element_type=F32)


def layer(
    nodes,
    groups,
    tok_hbm,
    ids_hbm,
    rw_hbm,
    wg_hbm,
    wu_hbm,
    wd_hbm,
    out_ref,
    ids_ref,
    rw_ref,
    tok,
    wg,
    wu,
    wd,
    sbuf,
    rbuf,
    xbuf,
    wsb,
    wrb,
    wx,
    wcol,
    acc,
    hid,
    opp,
    opp_in,
    near,
    near_in,
    rsb,
    rrb,
    zbuf,
    zin,
    wbuf,
    win,
    w_opp_in,
    w_near,
    w_near_in,
    place_ref,
    place_t_ref,
    sems,
    round_sem,
):
    chunks, rows_tok, width = tok.shape
    plain = chunks - 1
    steps = BATCHES * plain
    some = groups // BATCHES
    slots = groups * CAP
    rows = some * CAP
    half = rows // 2
    ff = wg.shape[2]
    me_n = lax.axis_index("node")
    me_t = lax.axis_index("torus")
    right = (lax.rem(me_n + 1, nodes), me_t)
    left = (lax.rem(me_n + nodes - 1, nodes), me_t)
    OWN, RIGHT, LEFT, FAR = range(4)

    table = steps + 1 + BATCHES

    def plane_in(u):
        return sems.at[u]

    def near_sem(u):
        return sems.at[table + u]

    def far_sem(u):
        return sems.at[2 * table + u]

    def back_sem(c):
        return sems.at[3 * table + c]

    def single(k):
        return sems.at[3 * table + plain + BATCHES + k]

    def plane_peer(r):
        return (me_n, lax.rem(me_t + r, groups))

    def remote(src, dst, send, recv, device):
        return pltpu.make_async_remote_copy(
            src_ref=src,
            dst_ref=dst,
            send_sem=send,
            recv_sem=recv,
            device_id=device,
            device_id_type=MESH,
        )

    def spread(src, dst, send, recv, batch, base=0):
        def one(j, carry):
            peer = plane_peer(BATCHES * j + batch)
            remote(src.at[base + j], dst.at[base + some - batch - j], send, recv, peer).start()
            return carry

        lax.fori_loop(1 - batch, some, one, 0)

    def spread_desc(src, dst, send, recv, low, high):
        at = pl.ds(low, high - low)
        return remote(src.at[at], dst.at[at], send, recv, plane_peer(1))

    def plane_sent(batch):
        return single(PLANE_SENT) if batch == 0 else single(PLANE_SENT_ODD)

    across = min(4, groups // 2)
    deep = groups // (2 * across)
    me_core, me_x, me_z = lax.rem(me_t, 2), lax.rem(me_t // 2, across), me_t // (2 * across)

    def torus_peer(dz, dx, dc):
        z, x, core = lax.rem(me_z + dz, deep), lax.rem(me_x + dx, across), lax.rem(me_core + dc, 2)
        return (me_n, (z * across + x) * 2 + core)

    beside = [torus_peer(0, dx, 0) for dx in range(1, across)]
    greeted = [right, left, torus_peer(0, 0, 1)] + beside
    greeted += [torus_peer(0, dx, 1) for dx in range(1, across)]
    greeted += [torus_peer(dz, 0, dc) for dz in range(1, deep) for dc in range(2)]
    barrier = pltpu.get_barrier_semaphore()
    for device in greeted:
        pl.semaphore_signal(barrier, inc=1, device_id=device, device_id_type=MESH)

    def tok_copy(c):
        return pltpu.make_async_copy(
            tok_hbm.at[:, pl.ds(pl.multiple_of(c * width, width), width)],
            tok.at[c],
            single(TOK_FIRST if c == 0 else TOK_REST),
        )

    def wd_copy(c):
        return pltpu.make_async_copy(
            wd_hbm.at[:, pl.ds(pl.multiple_of(c * width, width), width)], wd.at[c], single(W_DOWN)
        )

    wg_copy = pltpu.make_async_copy(wg_hbm, wg, single(W_GATE))
    wu_copy = pltpu.make_async_copy(wu_hbm, wu, single(W_UP))
    ids_copy = pltpu.make_async_copy(ids_hbm, ids_ref, single(IDS))
    rw_copy = pltpu.make_async_copy(rw_hbm, rw_ref, single(GAINS))
    ids_copy.start()
    rw_copy.start()
    for c in range(chunks):
        tok_copy(c).start()
    wg_copy.start()
    wu_copy.start()
    for c in range(chunks):
        wd_copy(c).start()

    slot = lax.broadcasted_iota(jnp.int32, (slots, rows_tok), 0)
    spot = slot // CAP
    offset = BATCHES * lax.rem(spot, some) + spot // some
    group = lax.rem(me_t + offset, groups)
    ids_copy.wait()
    rw_copy.wait()
    ids = ids_ref[...]
    weights = rw_ref[...].astype(F32)
    member = jnp.zeros((slots, rows_tok), F32)
    weight_a = jnp.zeros((slots, rows_tok), F32)
    weight_b = jnp.zeros((slots, rows_tok), F32)
    for k in range(ids.shape[0]):
        one = jnp.broadcast_to(ids[k : k + 1, :], (slots, rows_tok))
        gain = jnp.broadcast_to(weights[k : k + 1, :], (slots, rows_tok))
        is_a = one == 2 * group
        is_b = one == 2 * group + 1
        weight_a = jnp.where(is_a, gain, weight_a)
        weight_b = jnp.where(is_b, gain, weight_b)
        member = jnp.where(is_a | is_b, jnp.float32(1.0), member)
    before = (
        lax.broadcasted_iota(jnp.int32, (rows_tok, rows_tok), 0)
        < lax.broadcasted_iota(jnp.int32, (rows_tok, rows_tok), 1)
    )
    before = jnp.where(before, jnp.float32(1.0), jnp.float32(0.0)).astype(BF16)
    index = dot(member.astype(BF16), before)
    here = index == lax.rem(slot, CAP).astype(F32)
    place = jnp.where(here, member, jnp.float32(0.0))
    place_ref[...] = place.astype(BF16)
    place_t_ref[...] = jnp.transpose(place).astype(BF16)
    lane = lax.broadcasted_iota(jnp.int32, (rows_tok, LANES), 1)
    low = jnp.where(lane < LANES // 2, jnp.float32(1.0), jnp.float32(0.0))
    spread_w = dot((place * weight_a).astype(BF16), low.astype(BF16)) + dot(
        (place * weight_b).astype(BF16), (1.0 - low).astype(BF16)
    )
    wsb[...] = spread_w.reshape(groups, CAP, LANES).astype(BF16)

    def prepare(c):
        if c == 0:
            tok_copy(0).wait()
        elif c == 1:
            rest = tok.at[pl.ds(1, chunks - 1)]
            pltpu.make_async_copy(rest, rest, single(TOK_REST)).wait()
        parts = []
        for b in range(width // QBLOCK):
            x = tok[c, :, b * QBLOCK : (b + 1) * QBLOCK].astype(F32)
            top = jnp.max(jnp.abs(x), axis=1, keepdims=True)
            scale = ((top + 1e-06) * (1.0 / 448.0)).astype(BF16).astype(F32)
            scale = jnp.broadcast_to(scale, x.shape)
            quantized = (x / scale).astype(BF16)
            parts.append((quantized.astype(F32) * scale).astype(BF16))
        restored = jnp.concatenate(parts, axis=1)
        picked = dot(place_ref[...], restored).reshape(groups, CAP, width).astype(BF16)
        if c == 0:
            zbuf[OWN] = picked
        else:
            for b in range(BATCHES):
                sbuf[b * plain + c - 1] = picked[b * some : (b + 1) * some]

    def send_plane(u):
        if isinstance(u, int):
            spread(sbuf.at[u], rbuf.at[u], plane_sent(u // plain), plane_in(u), u // plain)
            return
        for b in range(BATCHES):

            @pl.when(u // plain == b)
            def _(b=b):
                spread(sbuf.at[u], rbuf.at[u], plane_sent(b), plane_in(u), b)

    def y_send(block, u, sent):
        return (
            remote(block.at[OWN], block.at[LEFT], single(sent), near_sem(u), right),
            remote(block.at[OWN], block.at[RIGHT], single(sent), near_sem(u), left),
        )

    def y_relay(block, u, sent):
        middle = block.shape[1] // 2
        low, high = pl.ds(0, middle), pl.ds(middle, middle)
        return (
            remote(block.at[LEFT, low], block.at[FAR, low], single(sent), far_sem(u), right),
            remote(block.at[RIGHT, high], block.at[FAR, high], single(sent), far_sem(u), left),
        )

    def wait_in(ref, sem):
        remote(ref, ref, single(Y_SENT), sem, right).wait_recv()

    def wait_out(ref, k):
        remote(ref, ref, single(k), near_sem(0), right).wait_send()

    def wait_far(block, u):
        wait_in(block.at[FAR], far_sem(u))

    def flat(ref_value):
        count, cap, lanes = ref_value.shape
        return ref_value.astype(F32).reshape(count * cap, lanes).astype(BF16)

    def arrive(u):
        def gather(low, high):
            wait_in(rbuf.at[u, pl.ds(low, high - low)], plane_in(u))

        def own_too():
            gather(1, some)
            rbuf[u, 0] = sbuf[u, 0]

        if isinstance(u, int):
            own_too()
        else:
            pl.when(u // plain == 0)(own_too)
            pl.when(u // plain == 1)(lambda: gather(0, some))
        xbuf[u, OWN] = flat(rbuf[u])
        for copy in y_send(xbuf.at[u], u, Y_SENT):
            copy.start()

    def pass_on(block, u, sent):
        wait_in(block.at[pl.ds(RIGHT, 2)], near_sem(u))
        for copy in y_relay(block, u, sent):
            copy.start()

    def multiply(u):
        wait_far(xbuf.at[u], u)
        batch = u // plain
        add_chunk(xbuf[u].reshape(nodes * rows, width), batch, u - batch * plain + 1)

    def add_chunk(x, batch, c):
        at = pl.ds(pl.multiple_of(c * width, width), width)
        for e in range(EXP_DEV):
            acc[batch, 2 * e] += dot(x, wg[e, at, :])
            acc[batch, 2 * e + 1] += dot(x, wu[e, at, :])

    def z_piece(batch):
        return zbuf.at[:, pl.ds(batch * some, some)], steps + 1 + batch

    def spread_planes(src, dst, send, recv, batch):
        def one(j, carry):
            peer = plane_peer(BATCHES * j + batch)
            here, there = batch * some + j, batch * some + some - batch - j
            remote(src.at[:, here], dst.at[:, there], send, recv, peer).start()
            return carry

        lax.fori_loop(1 - batch, some, one, 0)

    def wait_planes(ref, sem, batch):
        wait_in(ref.at[:, pl.ds(batch * some + 1 - batch, some - 1 + batch)], sem)

    def z_out(batch):
        wait_far(*z_piece(batch))
        spread_planes(zbuf, zin, single(Z_PLANE_SENT), plane_in(steps + 1 + batch), batch)

    def z_multiply(batch):
        wait_planes(zin, plane_in(steps + 1 + batch), batch)
        if batch == 0:
            zin[:, 0] = zbuf[:, 0]
        x = zin[:, batch * some : (batch + 1) * some].astype(F32)
        add_chunk(x.reshape(nodes * rows, width).astype(BF16), batch, 0)

    def w_project(batch):
        part = dot(hid[batch], wd[plain])
        wbuf[:, batch * some : (batch + 1) * some] = part.reshape(nodes, some, CAP, width).astype(BF16)
        spread_planes(wbuf, win, single(W_PLANE_SENT), back_sem(plain + batch), batch)

    def w_opposite(batch):
        wait_planes(win, back_sem(plain + batch), batch)
        if batch == 0:
            win[:, 0] = wbuf[:, 0]
        mid = some // 2
        for k, device in enumerate((right, left)):
            part = win.at[FAR, pl.ds(batch * some + k * mid, mid)]
            sem = near_sem(steps + 1 + batch)
            remote(part, w_opp_in.at[batch, k], single(W_FAR_SENT), sem, device).start()

    def w_neighbour(batch):
        low, mid, high = batch * some, batch * some + some // 2, (batch + 1) * some
        wait_in(w_opp_in.at[batch], near_sem(steps + 1 + batch))
        w_near[batch, 0, : some // 2] = (
            win[RIGHT, low:mid].astype(F32) + w_opp_in[batch, 0].astype(F32)
        ).astype(BF16)
        w_near[batch, 0, some // 2 :] = win[RIGHT, mid:high]
        w_near[batch, 1, : some // 2] = win[LEFT, low:mid]
        w_near[batch, 1, some // 2 :] = (
            win[LEFT, mid:high].astype(F32) + w_opp_in[batch, 1].astype(F32)
        ).astype(BF16)
        for k, device in enumerate((right, left)):
            sem = far_sem(steps + 1 + batch)
            remote(w_near.at[batch, k], w_near_in.at[batch, k], single(W_NEAR_SENT), sem, device).start()

    def w_finish(batch):
        wait_in(w_near_in.at[batch], far_sem(steps + 1 + batch))
        part = win[OWN, batch * some : (batch + 1) * some].astype(F32)
        part = part + w_near_in[batch, 0].astype(F32) + w_near_in[batch, 1].astype(F32)
        return dot(
            place_t_ref[:, batch * rows : (batch + 1) * rows], part.reshape(rows, width).astype(BF16)
        )

    def activate(batch):
        for e in range(EXP_DEV):
            gate = acc[batch, 2 * e]
            gain = wcol[e, :, batch * rows : (batch + 1) * rows, :].reshape(nodes * rows, LANES)
            gain = jnp.broadcast_to(gain[:, :1], gate.shape)
            value = gate / (1.0 + jnp.exp(-gate)) * acc[batch, 2 * e + 1] * gain
            hid[batch, :, e * ff : (e + 1) * ff] = value.astype(BF16)

    def project(u, first, count):
        batch = u // plain
        return dot(hid[batch, first * rows : (first + count) * rows, :], wd[u - batch * plain])

    def start_opposite(u):
        part = project(u, FAR, 1)
        for k, device in enumerate((right, left)):
            opp[u, k] = part[k * half : (k + 1) * half].astype(BF16)
            remote(opp.at[u, k], opp_in.at[u, k], single(OPP_SENT), near_sem(u), device).start()

    def start_neighbour(u):
        part = project(u, RIGHT, 2)
        wait_in(opp_in.at[u], near_sem(u))
        near[u, 0, :half] = (part[:half] + opp_in[u, 0].astype(F32)).astype(BF16)
        near[u, 0, half:] = part[half:rows].astype(BF16)
        near[u, 1, :half] = part[rows : rows + half].astype(BF16)
        near[u, 1, half:] = (part[rows + half :] + opp_in[u, 1].astype(F32)).astype(BF16)
        for k, device in enumerate((right, left)):
            remote(near.at[u, k], near_in.at[u, k], single(NEAR_SENT), far_sem(u), device).start()

    def finish(u):
        part = project(u, OWN, 1)
        wait_in(near_in.at[u], far_sem(u))
        part = part + near_in[u, 0].astype(F32) + near_in[u, 1].astype(F32)
        batch = u // plain
        c, base = u - batch * plain, batch * some
        rsb[c, pl.ds(base, some)] = part.reshape(some, CAP, width).astype(BF16)
        spread(rsb.at[c], rrb.at[c], single(BACK_SENT), back_sem(c), batch, base)

    def collect(c):
        wait_in(rrb.at[c, pl.ds(1, groups - 1)], back_sem(c))
        rrb[c, 0] = rsb[c, 0]
        total = jnp.zeros((rows_tok, width), F32)
        for b in range(BATCHES):
            back = flat(rrb[c, b * some : (b + 1) * some])
            total += dot(place_t_ref[:, b * rows : (b + 1) * rows], back)
        out_ref[:, pl.ds(pl.multiple_of(c * width, width), width)] = total.astype(BF16)

    prepare(0)
    pl.semaphore_wait(barrier, len(greeted))
    for b in range(BATCHES):
        for copy in y_send(*z_piece(b), Z_Y_SENT):
            copy.start()
    acc[...] = jnp.zeros_like(acc)
    for device in beside:
        pl.semaphore_signal(round_sem, inc=1, device_id=device, device_id_type=MESH)
    prepare(1)
    pl.semaphore_wait(round_sem, len(beside))
    for c in range(2, chunks):
        if c - 2 < EARLY:
            send_plane(c - 2)
        prepare(c)
        if c == 4:
            pass_on(*z_piece(0), Z_RELAY_SENT)
    for b in range(BATCHES):
        at = pl.ds(b * some, some)
        spread(wsb.at[at], wrb.at[at], single(GAIN_PLANE_SENT), plane_in(steps), b)
    arrive(0)
    pass_on(*z_piece(1), Z_RELAY_SENT)

    lag_y, lag_x, lag_m = 0, 2, 4
    lag_o = steps
    lag_n, lag_f, lag_c = lag_o + 2, lag_o + 4, lag_o + 6

    def stage(s, lag, first, last, work):
        @pl.when((s >= lag + first) & (s < lag + last))
        def _():
            work(s - lag)

    def at_step(s, step, work, *args):
        @pl.when(s == step)
        def _():
            work(*args)

    def share_weights():
        wait_in(wrb.at[pl.ds(1, groups - 1)], plane_in(steps))
        wrb[0] = wsb[0]
        turned = jnp.transpose(wrb[...].astype(F32).reshape(slots, LANES)).astype(BF16)
        for e in range(EXP_DEV):
            first = e * (LANES // EXP_DEV)
            wx[OWN, e * PACK : (e + 1) * PACK] = turned[first : first + PACK]
        for copy in y_send(wx, steps, GAIN_Y_SENT):
            copy.start()

    def have_gate_up():
        wg_copy.wait()
        wu_copy.wait()
        pltpu.make_async_copy(wd, wd, single(W_DOWN)).wait()

    def have_weights():
        wait_far(wx, steps)
        for e in range(EXP_DEV):
            for plane in range(nodes):
                line = wx[plane, e * PACK : e * PACK + 1, :].astype(F32)
                wcol[e, plane] = jnp.transpose(jnp.broadcast_to(line, (LANES, slots)))

    def turn(batch):
        z_multiply(batch)
        activate(batch)
        w_project(batch)

    def w_last():
        total = w_finish(0) + w_finish(1)
        out_ref[:, plain * width :] = total.astype(BF16)

    def send_two(k):
        send_plane(EARLY + 2 * k)
        send_plane(EARLY + 1 + 2 * k)

    def whole(s, carry):
        stage(s, 0, 0, (steps - EARLY) // 2, send_two)
        stage(s, lag_y, 1, steps, arrive)
        at_step(s, 3, share_weights)
        at_step(s, 3, have_gate_up)
        stage(s, lag_x, 0, steps, lambda u: pass_on(xbuf.at[u], u, RELAY_SENT))
        at_step(s, 5, pass_on, wx, steps, GAIN_RELAY_SENT)
        at_step(s, 4, z_out, 0)
        at_step(s, 5, z_out, 1)
        stage(s, lag_m, 0, steps, multiply)
        at_step(s, 8, have_weights)
        at_step(s, steps, turn, 0)
        at_step(s, lag_m + steps - 1, turn, 1)
        stage(s, lag_o, 0, steps, start_opposite)
        at_step(s, lag_o + steps, w_opposite, 0)
        stage(s, lag_n, 0, steps, start_neighbour)
        at_step(s, lag_o + steps + 1, w_opposite, 1)
        at_step(s, lag_n + steps, w_neighbour, 0)
        stage(s, lag_f, 0, steps, finish)
        at_step(s, lag_n + steps + 1, w_neighbour, 1)
        stage(s, lag_c + steps - plain, 0, plain, collect)
        at_step(s, lag_f + steps + 1, w_last)
        return carry

    lax.fori_loop(0, lag_f + steps + 2, whole, 0)

    first, second = pl.ds(0, plain), pl.ds(plain, plain)
    wait_out(sbuf.at[first, pl.ds(1, some - 1)], PLANE_SENT)
    wait_out(sbuf.at[second], PLANE_SENT_ODD)
    wait_out(wsb.at[pl.ds(1, groups - 1)], GAIN_PLANE_SENT)
    wait_out(zbuf.at[:, pl.ds(1, groups - 1)], Z_PLANE_SENT)
    wait_out(wbuf.at[:, pl.ds(1, groups - 1)], W_PLANE_SENT)
    wait_out(rsb.at[:, pl.ds(1, groups - 1)], BACK_SENT)
    wait_out(xbuf.at[:, pl.ds(RIGHT, 2)], Y_SENT)
    wait_out(xbuf.at[:, FAR], RELAY_SENT)
    wait_out(wx.at[pl.ds(RIGHT, 2)], GAIN_Y_SENT)
    wait_out(wx.at[FAR], GAIN_RELAY_SENT)
    wait_out(zbuf.at[pl.ds(RIGHT, 2)], Z_Y_SENT)
    wait_out(zbuf.at[FAR], Z_RELAY_SENT)
    wait_out(opp, OPP_SENT)
    wait_out(near, NEAR_SENT)
    wait_out(w_opp_in, W_FAR_SENT)
    wait_out(w_near, W_NEAR_SENT)


def solution(mesh):
    nodes, groups = mesh.shape["node"], mesh.shape["torus"]

    def shards(tokens, expert_ids, route_weight, w_gate, w_up, w_down):
        rows_tok, depth = tokens.shape
        ff = w_gate.shape[2]
        width = min(CHUNK, depth)
        chunks = depth // width
        slots = groups * CAP
        steps = BATCHES * (chunks - 1)
        some = groups // BATCHES
        rows = some * CAP
        anywhere = pl.BlockSpec(memory_space=pl.ANY)
        inside = pl.BlockSpec(memory_space=pltpu.VMEM)
        block = pltpu.VMEM((steps, some, CAP, width), BF16)
        planes = pltpu.VMEM((nodes, groups, CAP, width), BF16)
        piece = pltpu.VMEM((BATCHES, 2, some, CAP, width), BF16)
        returned = pltpu.VMEM((chunks - 1, groups, CAP, width), BF16)
        arrivals = 3 * (steps + 1 + BATCHES) + chunks - 1 + BATCHES
        return pl.pallas_call(
            functools.partial(layer, nodes, groups),
            out_shape=pltpu.VMEM((rows_tok, depth), BF16),
            in_specs=[anywhere] * 6,
            out_specs=inside,
            scratch_shapes=[
                pltpu.VMEM(expert_ids.shape[::-1], jnp.int32),
                pltpu.VMEM(route_weight.shape[::-1], BF16),
                pltpu.VMEM((chunks, rows_tok, width), BF16),
                pltpu.VMEM(w_gate.shape, BF16),
                pltpu.VMEM(w_up.shape, BF16),
                pltpu.VMEM((chunks, EXP_DEV * ff, width), BF16),
                block,
                block,
                pltpu.VMEM((steps, nodes, rows, width), BF16),
                pltpu.VMEM((groups, CAP, LANES), BF16),
                pltpu.VMEM((groups, CAP, LANES), BF16),
                pltpu.VMEM((nodes, EXP_DEV * PACK, slots), BF16),
                pltpu.VMEM((EXP_DEV, nodes, slots, LANES), F32),
                pltpu.VMEM((BATCHES, 2 * EXP_DEV, nodes * rows, ff), F32),
                pltpu.VMEM((BATCHES, nodes * rows, EXP_DEV * ff), BF16),
                pltpu.VMEM((steps, 2, rows // 2, width), BF16),
                pltpu.VMEM((steps, 2, rows // 2, width), BF16),
                pltpu.VMEM((steps, 2, rows, width), BF16),
                pltpu.VMEM((steps, 2, rows, width), BF16),
                returned,
                returned,
                planes,
                planes,
                planes,
                planes,
                pltpu.VMEM((BATCHES, 2, some // 2, CAP, width), BF16),
                piece,
                piece,
                pltpu.VMEM((slots, rows_tok), BF16),
                pltpu.VMEM((rows_tok, slots), BF16),
                pltpu.SemaphoreType.DMA((arrivals + SINGLES,)),
                pltpu.SemaphoreType.REGULAR,
            ],
            compiler_params=pltpu.CompilerParams(
                collective_id=0, has_side_effects=True, vmem_limit_bytes=59000000
            ),
        )(
            tokens,
            expert_ids.T,
            route_weight.T,
            w_gate,
            w_up,
            w_down.reshape(EXP_DEV * ff, depth),
        )

    placed = (
        P(("node", "torus"), None),
        P(("node", "torus"), None),
        P(("node", "torus"), None),
        P("torus", None, "node"),
        P("torus", None, "node"),
        P("torus", "node", None),
    )
    return jax.shard_map(
        shards, mesh=mesh, in_specs=placed, out_specs=P(("node", "torus"), None), check_vma=False
    )
```
